8 devices in a mesh: dp: 1 (over z), tp: 8 (over y, x, core).
Axes of the slice: x: 2, y: 2, z: 1, core: 2. Of those that a mesh axis runs over, the one named last changes fastest.
Arguments:
- x_seq: bfloat16 [3, 256, 5120], P(None, 'dp')
- cache_len: int32 [256], P('dp')
- k_cache: bfloat16 [256, 8, 256, 128], P('dp', 'tp')
- v_cache: bfloat16 [256, 8, 256, 128], P('dp', 'tp')
- w_q: bfloat16 [5120, 5120], P(None, 'tp')
- w_k: bfloat16 [5120, 1024], P(None, 'tp')
- w_v: bfloat16 [5120, 1024], P(None, 'tp')
- w_o: bfloat16 [5120, 5120], P('tp')
- w_gate: bfloat16 [5120, 27648], P(None, 'tp')
- w_up: bfloat16 [5120, 27648], P(None, 'tp')
- w_down: bfloat16 [27648, 5120], P('tp')
- g_q: bfloat16 [5120], P('tp')
- g_k: bfloat16 [1024], P('tp')
- g_attn: bfloat16 [5120], replicated
- g_mlp: bfloat16 [5120], replicated
Outputs:
- output 1: bfloat16 [3, 256, 5120], P(None, 'dp')
- output 2: bfloat16 [256, 8, 256, 128], P('dp', 'tp')
- output 3: bfloat16 [256, 8, 256, 128], P('dp', 'tp')
All inputs are finite; a program needn't handle non-finite values.
Results may differ from the reference program's by a relative error of at most 0.02.
Values are sent between devices in bfloat16 or wider.
A program may use at most 1 GiB of HBM per device.

```python
import math
import jax
import jax.numpy as jnp
from jax import lax

STEPS = 3
MIN_LEN = 128
D_MODEL = 5120
N_HEADS = 40
N_KV_HEADS = 8
HEAD_DIM = 128
FF_DIM = 27648
BATCH_ROWS = 256
MAX_SEQ = 256
ROPE_THETA = 500000.0
NORM_EPS = 1e-6


def draw_lengths(len_key):
    sub_keys = jax.random.split(len_key, 3)
    lengths = jax.random.randint(sub_keys[0], (BATCH_ROWS,), MIN_LEN, MAX_SEQ - STEPS + 1)
    long_row = jax.random.randint(sub_keys[1], (), 0, BATCH_ROWS)
    short_row = (long_row + 1 + jax.random.randint(sub_keys[2], (), 0, BATCH_ROWS - 1)) % BATCH_ROWS
    lengths = lengths.at[long_row].set(MAX_SEQ - STEPS).at[short_row].set(MIN_LEN)
    return lengths.astype(jnp.int32)


def normal_weight(w_key, rows_in, cols_out):
    return jax.random.normal(w_key, (rows_in, cols_out), jnp.float32) * rows_in ** -0.5


def head_scales(scale_key, n_heads):
    log_scale = jax.random.uniform(scale_key, (n_heads,), jnp.float32, math.log(0.3), math.log(3.0))
    return jnp.repeat(jnp.exp(log_scale), HEAD_DIM)


def setup_inputs(seed: int = 0, part: int = 0) -> dict:
    base_key = jax.random.key(seed)
    part_keys = jax.random.split(jax.random.fold_in(base_key, part), 4)
    w_keys = jax.random.split(jax.random.key(seed + 1), 13)
    q_width = N_HEADS * HEAD_DIM
    kv_width = N_KV_HEADS * HEAD_DIM
    cache_shape = (BATCH_ROWS, N_KV_HEADS, MAX_SEQ, HEAD_DIM)
    x_seq = jax.random.normal(part_keys[0], (STEPS, BATCH_ROWS, D_MODEL), jnp.float32)
    k_cache = jax.random.normal(part_keys[2], cache_shape, jnp.float32)
    v_cache = jax.random.normal(part_keys[3], cache_shape, jnp.float32)
    w_q = normal_weight(w_keys[0], D_MODEL, q_width) * head_scales(w_keys[1], N_HEADS)[None, :]
    w_k = normal_weight(w_keys[2], D_MODEL, kv_width) * head_scales(w_keys[3], N_KV_HEADS)[None, :]
    w_v = normal_weight(w_keys[4], D_MODEL, kv_width)
    w_o = normal_weight(w_keys[5], q_width, D_MODEL)
    w_gate = normal_weight(w_keys[6], D_MODEL, FF_DIM)
    w_up = normal_weight(w_keys[7], D_MODEL, FF_DIM)
    w_down = normal_weight(w_keys[8], FF_DIM, D_MODEL)
    g_q = jax.random.uniform(w_keys[9], (q_width,), jnp.float32, 0.5, 1.5)
    g_k = jax.random.uniform(w_keys[10], (kv_width,), jnp.float32, 0.5, 1.5)
    g_attn = jax.random.uniform(w_keys[11], (D_MODEL,), jnp.float32, 0.5, 1.5)
    g_mlp = jax.random.uniform(w_keys[12], (D_MODEL,), jnp.float32, 0.5, 1.5)
    return {'x_seq': x_seq.astype(jnp.bfloat16), 'cache_len': draw_lengths(part_keys[1]), 'k_cache': k_cache.astype(jnp.bfloat16), 'v_cache': v_cache.astype(jnp.bfloat16), 'w_q': w_q.astype(jnp.bfloat16), 'w_k': w_k.astype(jnp.bfloat16), 'w_v': w_v.astype(jnp.bfloat16), 'w_o': w_o.astype(jnp.bfloat16), 'w_gate': w_gate.astype(jnp.bfloat16), 'w_up': w_up.astype(jnp.bfloat16), 'w_down': w_down.astype(jnp.bfloat16), 'g_q': g_q.astype(jnp.bfloat16), 'g_k': g_k.astype(jnp.bfloat16), 'g_attn': g_attn.astype(jnp.bfloat16), 'g_mlp': g_mlp.astype(jnp.bfloat16)}


def rms_factor(sq_sum, full_width):
    return lax.rsqrt(sq_sum / full_width + NORM_EPS)


def rope_tables(positions):
    half_dim = HEAD_DIM // 2
    inv_freq = ROPE_THETA ** (-(jnp.arange(half_dim, dtype=jnp.float32) * (2.0 / HEAD_DIM)))
    angles = positions.astype(jnp.float32)[:, None] * inv_freq[None, :]
    return jnp.cos(angles), jnp.sin(angles)


def apply_rope(head_vals, cos_tab, sin_tab):
    half_dim = HEAD_DIM // 2
    lead_half = head_vals[..., :half_dim]
    tail_half = head_vals[..., half_dim:]
    cos_rows = cos_tab[:, None, :]
    sin_rows = sin_tab[:, None, :]
    return jnp.concatenate([lead_half * cos_rows - tail_half * sin_rows, tail_half * cos_rows + lead_half * sin_rows], axis=-1)


def reference(x_seq, cache_len, k_cache, v_cache, w_q, w_k, w_v, w_o, w_gate, w_up, w_down, g_q, g_k, g_attn, g_mlp):
    q_width = N_HEADS * HEAD_DIM
    kv_width = N_KV_HEADS * HEAD_DIM
    group_size = N_HEADS // N_KV_HEADS
    row_ids = jnp.arange(BATCH_ROWS)
    seq_ids = jnp.arange(MAX_SEQ)
    gain_q = g_q.astype(jnp.float32)
    gain_k = g_k.astype(jnp.float32)
    gain_a = g_attn.astype(jnp.float32)
    gain_m = g_mlp.astype(jnp.float32)

    def attend_row(row_in):
        q_row, k_row, v_row, last_pos = row_in
        q_grp = q_row.reshape(N_KV_HEADS, group_size, HEAD_DIM).astype(jnp.float32)
        scores = jnp.einsum('kgd,ksd->kgs', q_grp, k_row.astype(jnp.float32)) * HEAD_DIM ** -0.5
        scores = jnp.where(seq_ids <= last_pos, scores, -jnp.inf)
        row_max = jnp.max(scores, axis=-1, keepdims=True)
        exp_scores = jnp.exp(scores - row_max)
        row_sum = jnp.sum(exp_scores, axis=-1, keepdims=True)
        mixed_vals = jnp.einsum('kgs,ksd->kgd', exp_scores.astype(jnp.bfloat16).astype(jnp.float32), v_row.astype(jnp.float32))
        return (mixed_vals / row_sum).astype(jnp.bfloat16).reshape(q_width)

    def one_step(cache_pair, step_in):
        k_all, v_all = cache_pair
        x_tok, step_idx = step_in
        positions = cache_len + step_idx
        q_raw = jnp.dot(x_tok, w_q, preferred_element_type=jnp.float32).astype(jnp.bfloat16).astype(jnp.float32)
        k_raw = jnp.dot(x_tok, w_k, preferred_element_type=jnp.float32).astype(jnp.bfloat16).astype(jnp.float32)
        v_new = jnp.dot(x_tok, w_v, preferred_element_type=jnp.float32).astype(jnp.bfloat16).reshape(BATCH_ROWS, N_KV_HEADS, HEAD_DIM)
        q_normed = q_raw * rms_factor(jnp.sum(q_raw * q_raw, axis=-1, keepdims=True), q_width) * gain_q
        k_normed = k_raw * rms_factor(jnp.sum(k_raw * k_raw, axis=-1, keepdims=True), kv_width) * gain_k
        cos_tab, sin_tab = rope_tables(positions)
        q_rot = apply_rope(q_normed.reshape(BATCH_ROWS, N_HEADS, HEAD_DIM), cos_tab, sin_tab).astype(jnp.bfloat16)
        k_rot = apply_rope(k_normed.reshape(BATCH_ROWS, N_KV_HEADS, HEAD_DIM), cos_tab, sin_tab).astype(jnp.bfloat16)
        k_all = k_all.at[row_ids, :, positions, :].set(k_rot)
        v_all = v_all.at[row_ids, :, positions, :].set(v_new)
        attn_vals = lax.map(attend_row, (q_rot, k_all, v_all, positions))
        attn_sum = jnp.dot(attn_vals, w_o, preferred_element_type=jnp.float32).astype(jnp.bfloat16).astype(jnp.float32)
        hidden = (x_tok.astype(jnp.float32) + attn_sum * rms_factor(jnp.sum(attn_sum * attn_sum, axis=-1, keepdims=True), D_MODEL) * gain_a).astype(jnp.bfloat16)
        gate_pre = jnp.dot(hidden, w_gate, preferred_element_type=jnp.float32)
        up_pre = jnp.dot(hidden, w_up, preferred_element_type=jnp.float32)
        act_vals = (jax.nn.silu(gate_pre) * up_pre).astype(jnp.bfloat16)
        mlp_sum = jnp.dot(act_vals, w_down, preferred_element_type=jnp.float32).astype(jnp.bfloat16).astype(jnp.float32)
        y_tok = (hidden.astype(jnp.float32) + mlp_sum * rms_factor(jnp.sum(mlp_sum * mlp_sum, axis=-1, keepdims=True), D_MODEL) * gain_m).astype(jnp.bfloat16)
        return (k_all, v_all), y_tok

    (k_final, v_final), y_seq = lax.scan(one_step, (k_cache, v_cache), (x_seq, jnp.arange(STEPS, dtype=jnp.int32)))
    return (y_seq, k_final, v_final)
```

```python
import functools

import jax
import jax.numpy as jnp
from jax import lax
from jax.experimental import pallas as pl
from jax.experimental.pallas import tpu as pltpu
from jax.sharding import PartitionSpec as P

ROPE_THETA = 500000.0
NORM_EPS = 1e-6
MESH_ID = pl.DeviceIdType.MESH
MIB = 2**20


def rms_factor(sq_sum, full_width):
    return lax.rsqrt(sq_sum / full_width + NORM_EPS)


def rope_tables(positions, head_dim):
    half_dim = head_dim // 2
    inv_freq = ROPE_THETA ** (-(jnp.arange(half_dim, dtype=jnp.float32) * (2.0 / head_dim)))
    angles = positions.astype(jnp.float32)[:, None] * inv_freq[None, :]
    return jnp.cos(angles), jnp.sin(angles)


def apply_rope(head_vals, cos_tab, sin_tab):
    half_dim = head_vals.shape[-1] // 2
    lead_half = head_vals[..., :half_dim]
    tail_half = head_vals[..., half_dim:]
    cos_rows = cos_tab[:, None, :]
    sin_rows = sin_tab[:, None, :]
    return jnp.concatenate([lead_half * cos_rows - tail_half * sin_rows, tail_half * cos_rows + lead_half * sin_rows], axis=-1)


def attend(q_rot, k_old, v_old, lengths, new_keys, new_vals):
    score_scale = q_rot.shape[-1] ** -0.5
    seq_max = k_old.shape[2]
    old_scores = jnp.einsum('bkgd,bksd->bkgs', q_rot, k_old, preferred_element_type=jnp.float32) * score_scale
    old_valid = jnp.arange(seq_max)[None, :] < lengths[:, None]
    old_scores = jnp.where(old_valid[:, None, None, :], old_scores, -jnp.inf)
    new_scores = jnp.einsum('bkgd,bktd->bkgt', q_rot, new_keys, preferred_element_type=jnp.float32) * score_scale
    row_max = jnp.maximum(jnp.max(old_scores, axis=-1, keepdims=True), jnp.max(new_scores, axis=-1, keepdims=True))
    old_exp = jnp.exp(old_scores - row_max)
    new_exp = jnp.exp(new_scores - row_max)
    row_sum = jnp.sum(old_exp, axis=-1, keepdims=True) + jnp.sum(new_exp, axis=-1, keepdims=True)
    mixed_vals = jnp.einsum('bkgs,bksd->bkgd', old_exp.astype(jnp.bfloat16), v_old, preferred_element_type=jnp.float32) + jnp.einsum('bkgt,bktd->bkgd', new_exp.astype(jnp.bfloat16), new_vals, preferred_element_type=jnp.float32)
    return (mixed_vals / row_sum).astype(jnp.bfloat16)


N_CB = 4
N_WB = 4
N_DB = 3
HB = 128
DB = 256


def tail_kernel(axis, o_hbm, x_hbm, wo_hbm, w1_hbm, w3_hbm, w2_hbm, ga_ref, gm_ref, y_hbm,
                ob, xp, hb, src, recv0, recv1, recv2, act, wob, wb, w2b,
                o_sem, x_sem, wo_sem, wb_sem, w2_sem, y_sem, s_sem, r_sem, g_ssem, g_rsem):
    n_steps, n_seq, d_model = x_hbm.shape
    half = n_seq // 2
    rows = n_steps * half
    piece = rows // 8
    cw = d_model // N_CB
    n_hid = w1_hbm.shape[1]
    n_j = n_hid // HB
    n_d = d_model // DB
    per_cb = n_d // N_CB

    me = lax.axis_index(axis)
    core = lax.rem(me, 2)
    xb = lax.rem(me // 2, 2)
    yb = me // 4
    first_bit = core * yb + (1 - core) * xb
    second_bit = core * xb + (1 - core) * yb
    fw = 1 + core
    sw = 2 - core
    partner = me + 1 - 2 * core
    fpeer = me + (1 - 2 * first_bit) * 2 * fw
    speer = me + (1 - 2 * second_bit) * 2 * sw
    fspeer = fpeer + speer - me

    def remote(src_ref, dst_ref, send, recv, dev):
        return pltpu.make_async_remote_copy(src_ref=src_ref, dst_ref=dst_ref, send_sem=send, recv_sem=recv, device_id={axis: dev}, device_id_type=MESH_ID)

    o_copy = pltpu.make_async_copy(o_hbm, ob, o_sem)
    o_copy.start()

    def wo_copy(cb):
        return pltpu.make_async_copy(wo_hbm.at[:, pl.ds(cb * cw, cw)], wob.at[:, pl.ds(cb * cw, cw)], wo_sem.at[cb])

    for cb in range(N_CB):
        wo_copy(cb).start()

    def x_copy(c, i):
        r0 = piece * me + 16 * i
        t = r0 // half
        b = pl.multiple_of(lax.rem(r0, half), 16)
        return pltpu.make_async_copy(x_hbm.at[t, pl.ds(c * half + b, 16), :], xp.at[c, pl.ds(16 * i, 16), :], x_sem.at[c, i])

    for c in range(2):
        for i in range(piece // 16):
            x_copy(c, i).start()

    def wb_copies(j, s):
        col = pl.ds(pl.multiple_of(j * HB, HB), HB)
        return (pltpu.make_async_copy(w1_hbm.at[:, col], wb.at[s, :, 0:HB], wb_sem.at[s, 0]),
                pltpu.make_async_copy(w3_hbm.at[:, col], wb.at[s, :, HB:2 * HB], wb_sem.at[s, 1]))

    def w2_copy(j, s):
        return pltpu.make_async_copy(w2_hbm.at[:, pl.ds(pl.multiple_of(j * DB, DB), DB)], w2b.at[s], w2_sem.at[s])

    for s in range(N_WB - 1):
        for cp in wb_copies(s, s):
            cp.start()

    bar = pltpu.get_barrier_semaphore()
    for dev in (partner, fpeer, speer):
        pl.semaphore_signal(bar, inc=1, device_id={axis: dev}, device_id_type=MESH_ID)
    pl.semaphore_wait(bar, 3)

    def cols_of(cb):
        return pl.ds(pl.multiple_of(cb * cw, cw), cw)

    def copy0(inst, cb):
        c = inst % 2
        return remote(src.at[c, :, 1 - core, :, cols_of(cb)], recv0.at[c, :, :, cols_of(cb)], s_sem.at[inst, 0, cb], r_sem.at[inst, 0, cb], partner)

    def copy1(inst, cb, k):
        c = inst % 2
        sb = (1 - second_bit) if k == 0 else second_bit
        idx = (1 - first_bit) * fw + sb * sw
        return remote(recv0.at[c, idx, :, cols_of(cb)], recv1.at[c, k, :, cols_of(cb)], s_sem.at[inst, 1 + k, cb], r_sem.at[inst, 1 + k, cb], fpeer)

    def copy2(inst, cb):
        c = inst % 2
        return remote(recv1.at[c, 0, :, cols_of(cb)], recv2.at[c, :, cols_of(cb)], s_sem.at[inst, 3, cb], r_sem.at[inst, 3, cb], speer)

    def f32(v):
        return v.astype(jnp.float32)

    def event1(inst, cb):
        c = inst % 2
        copy0(inst, cb).wait_recv()
        cols = cols_of(cb)

        def add(i, _):
            recv0[c, i, :, cols] = (f32(src[c, i, core, :, cols]) + f32(recv0[c, i, :, cols])).astype(jnp.bfloat16)
            return 0

        lax.fori_loop(0, 4, add, 0)
        copy1(inst, cb, 0).start()
        copy1(inst, cb, 1).start()

    def event2(inst, cb):
        c = inst % 2
        copy1(inst, cb, 0).wait_recv()
        cols = cols_of(cb)
        idx = first_bit * fw + (1 - second_bit) * sw
        recv1[c, 0, :, cols] = (f32(recv0[c, idx, :, cols]) + f32(recv1[c, 0, :, cols])).astype(jnp.bfloat16)
        copy2(inst, cb).start()

    def event3(inst, cb):
        c = inst % 2
        copy1(inst, cb, 1).wait_recv()
        copy2(inst, cb).wait_recv()
        cols = cols_of(cb)
        idx = first_bit * fw + second_bit * sw
        recv2[c, :, cols] = (f32(recv0[c, idx, :, cols]) + f32(recv1[c, 1, :, cols]) + f32(recv2[c, :, cols])).astype(jnp.bfloat16)

    def rows_of(c, dev):
        return hb.at[c, pl.ds(pl.multiple_of(dev * piece, 16), piece), :]

    def gcopy(inst, k):
        c = inst % 2
        who, dev = ((me, speer), (me, fpeer), (me, partner), (speer, fpeer), (speer, partner), (fpeer, partner), (fspeer, partner))[k]
        return remote(rows_of(c, who), rows_of(c, who), g_ssem.at[inst, k], g_rsem.at[inst, k], dev)

    def event4(inst):
        c = inst % 2
        gain_ref = ga_ref if inst < 2 else gm_ref

        def one(i, _):
            r = pl.ds(pl.multiple_of(i * 16, 16), 16)
            hr = pl.ds(pl.multiple_of(me * piece + i * 16, 16), 16)
            a = f32(recv2[c, r, :])
            factor = rms_factor(jnp.sum(a * a, axis=-1, keepdims=True), d_model)
            base = f32(xp[c, r, :]) if inst < 2 else f32(hb[c, hr, :])
            hb[c, hr, :] = (base + a * factor * f32(gain_ref[...])).astype(jnp.bfloat16)
            return 0

        lax.fori_loop(0, piece // 16, one, 0)

        def drain(cb, _):
            copy0(inst, cb).wait_send()
            copy1(inst, cb, 0).wait_send()
            copy1(inst, cb, 1).wait_send()
            copy2(inst, cb).wait_send()
            return 0

        lax.fori_loop(0, N_CB, drain, 0)
        for k in (1, 0, 2):
            gcopy(inst, k).start()

    def event5(inst):
        gcopy(inst, 0).wait_recv()
        gcopy(inst, 3).start()
        gcopy(inst, 4).start()

    def event6(inst):
        gcopy(inst, 1).wait_recv()
        gcopy(inst, 5).start()

    def event7(inst):
        gcopy(inst, 3).wait_recv()
        gcopy(inst, 6).start()

    def event8(inst):
        for k in (2, 4, 5, 6):
            gcopy(inst, k).wait_recv()
        for k in range(7):
            gcopy(inst, k).wait_send()

    def span(j, start, every, fn):
        k = j - start

        @pl.when((k >= 0) & (k < every * N_CB) & (lax.rem(k + every, every) == 0))
        def _():
            fn(k // every)

    def at(j, when, fn):
        @pl.when(j == when)
        def _():
            fn()

    def out_proj(c):
        def step(cb, _):
            part = jnp.dot(ob[c], wob[:, cols_of(cb)], preferred_element_type=jnp.float32).astype(jnp.bfloat16)
            src[c, :, :, :, cols_of(cb)] = part.reshape(4, 2, piece, cw)
            copy0(c, cb).start()
            return 0

        lax.fori_loop(0, N_CB, step, 0)

    def y_copies(c):
        return [pltpu.make_async_copy(hb.at[c, pl.ds(t * half, half), :], y_hbm.at[t, pl.ds(c * half, half), :], y_sem.at[c, t]) for t in range(n_steps)]

    o_copy.wait()
    for cb in range(N_CB):
        wo_copy(cb).wait()
    out_proj(0)
    lax.fori_loop(0, N_CB, lambda cb, _: (event1(0, cb), 0)[1], 0)
    out_proj(1)
    for c in range(2):
        for i in range(piece // 16):
            x_copy(c, i).wait()
    lax.fori_loop(0, N_CB, lambda cb, _: (event2(0, cb), 0)[1], 0)
    lax.fori_loop(0, N_CB, lambda cb, _: (event3(0, cb), 0)[1], 0)
    event4(0)
    event5(0)
    event6(0)
    event7(0)
    event8(0)

    for c in range(2):
        other = 1 + c

        def gate_up(j, _):
            s = lax.rem(j, N_WB)

            @pl.when(j + N_WB - 1 < n_j)
            def _():
                for cp in wb_copies(j + N_WB - 1, lax.rem(j + N_WB - 1, N_WB)):
                    cp.start()

            for cp in wb_copies(j, s):
                cp.wait()
            both = jnp.dot(hb[c], wb[s], preferred_element_type=jnp.float32)
            gate = both[:, :HB]
            act[:, pl.ds(pl.multiple_of(j * HB, HB), HB)] = (jax.nn.silu(gate) * both[:, HB:]).astype(jnp.bfloat16)
            span(j, 1, 1, functools.partial(event1, other))
            span(j, 6, 2, functools.partial(event2, other))
            span(j, 10, 2, functools.partial(event3, other))
            at(j, 17, functools.partial(event4, other))
            at(j, 24, functools.partial(event5, other))
            at(j, 25, functools.partial(event6, other))
            return 0

        for s in range(N_DB - 1):
            w2_copy(s, s).start()
        lax.fori_loop(0, n_j, gate_up, 0)
        if c == 0:
            for s in range(N_WB - 1):
                for cp in wb_copies(s, s):
                    cp.start()

        def down(j, _):
            s = lax.rem(j, N_DB)

            @pl.when(j + N_DB - 1 < n_d)
            def _():
                w2_copy(j + N_DB - 1, lax.rem(j + N_DB - 1, N_DB)).start()

            w2_copy(j, s).wait()
            part = jnp.dot(act[...], w2b[s], preferred_element_type=jnp.float32).astype(jnp.bfloat16)
            src[c, :, :, :, pl.ds(pl.multiple_of(j * DB, DB), DB)] = part.reshape(4, 2, piece, DB)

            @pl.when(lax.rem(j, per_cb) == per_cb - 1)
            def _():
                copy0(2 + c, j // per_cb).start()

            at(j, 7, functools.partial(event7, other))
            at(j, 10, functools.partial(event8, other))
            if c == 1:
                q = j // per_cb

                @pl.when(lax.rem(j, per_cb) == 2)
                def _():
                    @pl.when(q >= 1)
                    def _():
                        event1(3, q - 1)

                    @pl.when(q >= 2)
                    def _():
                        event2(3, q - 2)

                    @pl.when(q >= 3)
                    def _():
                        event3(3, q - 3)
            return 0

        lax.fori_loop(0, n_d, down, 0)
        if c == 1:
            for cp in y_copies(0):
                cp.start()

    event1(3, 3)
    event2(3, 2)
    event3(3, 1)
    event2(3, 3)
    event3(3, 2)
    event3(3, 3)
    event4(3)
    event5(3)
    event6(3)
    event7(3)
    event8(3)
    for cp in y_copies(1):
        cp.start()
    for c in range(2):
        for cp in y_copies(c):
            cp.wait()


def tail_layer(o, x_seq, w_o, w_gate, w_up, w_down, g_attn, g_mlp, axis):
    n_steps, n_seq, d_model = x_seq.shape
    rows = n_steps * n_seq // 2
    piece = rows // 8
    n_hid = w_gate.shape[1]
    bf16 = jnp.bfloat16
    anym = pl.BlockSpec(memory_space=pl.ANY)
    vmem = pl.BlockSpec(memory_space=pltpu.VMEM)
    dma = pltpu.SemaphoreType.DMA
    return pl.pallas_call(
        functools.partial(tail_kernel, axis),
        out_shape=jax.ShapeDtypeStruct((n_steps, n_seq, d_model), bf16),
        in_specs=[anym] * 6 + [vmem] * 2,
        out_specs=anym,
        scratch_shapes=[
            pltpu.VMEM((2, rows, w_o.shape[0]), bf16),
            pltpu.VMEM((2, piece, d_model), bf16),
            pltpu.VMEM((2, rows, d_model), bf16),
            pltpu.VMEM((2, 4, 2, piece, d_model), bf16),
            pltpu.VMEM((2, 4, piece, d_model), bf16),
            pltpu.VMEM((2, 2, piece, d_model), bf16),
            pltpu.VMEM((2, piece, d_model), bf16),
            pltpu.VMEM((rows, n_hid), bf16),
            pltpu.VMEM(w_o.shape, bf16),
            pltpu.VMEM((N_WB, d_model, 2 * HB), bf16),
            pltpu.VMEM((N_DB, n_hid, DB), bf16),
            dma, dma((2, piece // 16)), dma((N_CB,)), dma((N_WB, 2)), dma((N_DB,)), dma((2, n_steps)),
            dma((4, 4, N_CB)), dma((4, 4, N_CB)), dma((4, 7)), dma((4, 7)),
        ],
        compiler_params=pltpu.CompilerParams(collective_id=1, has_side_effects=True, vmem_limit_bytes=63 * MIB),
    )(o, x_seq, w_o, w_gate, w_up, w_down, g_attn.reshape(1, -1), g_mlp.reshape(1, -1))


def layer_steps(x_seq, cache_len, k_cache, v_cache, w_q, w_k, w_v, w_o, w_gate, w_up, w_down, g_q, g_k, g_attn, g_mlp, q_width, kv_width):
    num_steps, n_rows, d_model = x_seq.shape
    kv_loc = k_cache.shape[1]
    head_dim = k_cache.shape[-1]
    q_loc = w_q.shape[1] // head_dim
    group_size = q_loc // kv_loc
    gain_q = g_q.astype(jnp.float32)
    gain_k = g_k.astype(jnp.float32)
    new_keys = []
    new_vals = []
    o_list = []
    for step_idx in range(num_steps):
        x_tok = x_seq[step_idx]
        positions = cache_len + step_idx
        q_raw = jnp.dot(x_tok, w_q, preferred_element_type=jnp.float32).astype(jnp.bfloat16).astype(jnp.float32)
        k_raw = jnp.dot(x_tok, w_k, preferred_element_type=jnp.float32).astype(jnp.bfloat16).astype(jnp.float32)
        v_new = jnp.dot(x_tok, w_v, preferred_element_type=jnp.float32).astype(jnp.bfloat16)
        q_sq = lax.psum(jnp.sum(q_raw * q_raw, axis=-1, keepdims=True), 'tp')
        k_sq = lax.psum(jnp.sum(k_raw * k_raw, axis=-1, keepdims=True), 'tp')
        cos_tab, sin_tab = rope_tables(positions, head_dim)
        q_normed = (q_raw * rms_factor(q_sq, q_width) * gain_q).reshape(n_rows, q_loc, head_dim)
        k_normed = (k_raw * rms_factor(k_sq, kv_width) * gain_k).reshape(n_rows, kv_loc, head_dim)
        q_rot = apply_rope(q_normed, cos_tab, sin_tab).astype(jnp.bfloat16).reshape(n_rows, kv_loc, group_size, head_dim)
        new_keys.append(apply_rope(k_normed, cos_tab, sin_tab).astype(jnp.bfloat16))
        new_vals.append(v_new.reshape(n_rows, kv_loc, head_dim))
        attn_vals = attend(q_rot, k_cache, v_cache, cache_len, jnp.stack(new_keys, axis=2), jnp.stack(new_vals, axis=2))
        o_list.append(attn_vals.reshape(n_rows, q_loc * head_dim))
    o = jnp.stack(o_list).reshape(num_steps, 2, n_rows // 2, q_loc * head_dim).transpose(1, 0, 2, 3).reshape(2, num_steps * n_rows // 2, q_loc * head_dim)
    y = tail_layer(o, x_seq, w_o, w_gate, w_up, w_down, g_attn, g_mlp, 'tp')
    offsets = jnp.arange(k_cache.shape[2], dtype=jnp.int32)[None, None, :, None] - cache_len[:, None, None, None]
    k_out = k_cache
    v_out = v_cache
    for step_idx in range(num_steps):
        at_slot = offsets == step_idx
        k_out = jnp.where(at_slot, new_keys[step_idx][:, :, None, :], k_out)
        v_out = jnp.where(at_slot, new_vals[step_idx][:, :, None, :], v_out)
    return y, k_out, v_out


def solution(mesh):
    tp_size = mesh.shape['tp']

    def local_run(x_seq, cache_len, k_cache, v_cache, w_q, w_k, w_v, w_o, w_gate, w_up, w_down, g_q, g_k, g_attn, g_mlp):
        return layer_steps(x_seq, cache_len, k_cache, v_cache, w_q, w_k, w_v, w_o, w_gate, w_up, w_down, g_q, g_k, g_attn, g_mlp, w_q.shape[1] * tp_size, w_k.shape[1] * tp_size)

    data_spec = P(None, 'dp', None)
    cache_spec = P('dp', 'tp', None, None)
    col_spec = P(None, 'tp')
    row_spec = P('tp', None)
    arg_specs = (data_spec, P('dp'), cache_spec, cache_spec, col_spec, col_spec, col_spec, row_spec, col_spec, col_spec, row_spec, P('tp'), P('tp'), P(None), P(None))
    out_specs = (data_spec, cache_spec, cache_spec)
    return jax.shard_map(local_run, mesh=mesh, in_specs=arg_specs, out_specs=out_specs, check_vma=False)
```

```python
import functools

import jax
import jax.numpy as jnp
from jax import lax
from jax.experimental import pallas as pl
from jax.experimental.pallas import tpu as pltpu
from jax.sharding import PartitionSpec as P

ROPE_THETA = 500000.0
NORM_EPS = 1e-6
MESH_ID = pl.DeviceIdType.MESH
MIB = 2**20


def rms_factor(sq_sum, full_width):
    return lax.rsqrt(sq_sum / full_width + NORM_EPS)


N_KB = 5


def head_kernel(axis, q_width, kv_width, x_hbm, wq_hbm, wk_hbm, wv_hbm, gq_ref, gk_ref, len_ref, freq_ref, q_ref, kv_ref,
                xv, wv, acc, raw, sums, parts, in_sem, s_sem, r_sem):
    n_steps, n_seq, d_model = x_hbm.shape
    wq_cols = wq_hbm.shape[1]
    hd = wk_hbm.shape[1]
    n_heads = wq_cols // hd
    kw = d_model // N_KB
    n_blk = n_steps * 2
    me = lax.axis_index(axis)

    def in_copies(kb):
        ks = pl.ds(pl.multiple_of(kb * kw, kw), kw)
        return (pltpu.make_async_copy(x_hbm.at[:, :, ks], xv.at[:, :, ks], in_sem.at[kb, 0]),
                pltpu.make_async_copy(wq_hbm.at[ks, :], wv.at[ks, 0:wq_cols], in_sem.at[kb, 1]),
                pltpu.make_async_copy(wk_hbm.at[ks, :], wv.at[ks, wq_cols:wq_cols + hd], in_sem.at[kb, 2]),
                pltpu.make_async_copy(wv_hbm.at[ks, :], wv.at[ks, wq_cols + hd:wq_cols + 2 * hd], in_sem.at[kb, 3]))

    for kb in range(N_KB):
        for cp in in_copies(kb):
            cp.start()

    bar = pltpu.get_barrier_semaphore()
    for i in range(1, 8):
        pl.semaphore_signal(bar, inc=1, device_id={axis: lax.rem(me + i, 8)}, device_id_type=MESH_ID)

    def project(kb, _):
        for cp in in_copies(kb):
            cp.wait()
        ks = pl.ds(pl.multiple_of(kb * kw, kw), kw)
        for t in range(n_steps):
            part = jnp.dot(xv[t, :, ks], wv[ks, :], preferred_element_type=jnp.float32)

            @pl.when(kb == 0)
            def _():
                acc[t] = part

            @pl.when(kb > 0)
            def _():
                acc[t] += part
        return 0

    lax.fori_loop(0, N_KB, project, 0)

    lane = lax.broadcasted_iota(jnp.int32, (128, 128), 1)
    diag = lane == lax.broadcasted_iota(jnp.int32, (128, 128), 0)

    def to_row(col):
        return jnp.sum(jnp.where(diag, jnp.broadcast_to(col, (128, 128)), 0.0), axis=0, keepdims=True)

    def to_col(row):
        return jnp.sum(jnp.where(diag, jnp.broadcast_to(row, (128, 128)), 0.0), axis=1, keepdims=True)

    def rounded(v):
        return v.astype(jnp.bfloat16).astype(jnp.float32)

    sums[...] = jnp.zeros_like(sums)
    for blk in range(n_blk):
        t, half = blk // 2, blk % 2
        rows = slice(half * 128, half * 128 + 128)
        sq = None
        for g in range(n_heads):
            val = rounded(acc[t, rows, g * hd:(g + 1) * hd])
            raw[blk, g] = val
            sq = val * val if sq is None else sq + val * val
        sums[blk:blk + 1, :] = to_row(jnp.sum(sq, axis=-1, keepdims=True))
        val = rounded(acc[t, rows, wq_cols:wq_cols + hd])
        raw[blk, n_heads] = val
        sums[n_blk + blk:n_blk + blk + 1, :] = to_row(jnp.sum(val * val, axis=-1, keepdims=True))

    def exchange(i):
        return pltpu.make_async_remote_copy(src_ref=sums, dst_ref=parts.at[me], send_sem=s_sem.at[i - 1], recv_sem=r_sem.at[i - 1], device_id={axis: lax.rem(me + i, 8)}, device_id_type=MESH_ID)

    pl.semaphore_wait(bar, 7)
    for i in range(1, 8):
        exchange(i).start()
    parts[me] = sums[...]

    for blk in range(n_blk):
        t, half = blk // 2, blk % 2
        rows = slice(half * 128, half * 128 + 128)
        kv_ref[pl.ds(half * 1024 + 3 + t, 128, stride=8), :] = rounded(acc[t, rows, wq_cols + hd:wq_cols + 2 * hd])
    for half in range(2):
        zero = jnp.zeros((128, hd), jnp.float32)
        for slot in range(n_steps * n_heads, 16):
            q_ref[pl.ds(half * 2048 + slot, 128, stride=16), :] = zero
        for slot in range(2 * n_steps, 8):
            kv_ref[pl.ds(half * 1024 + slot, 128, stride=8), :] = zero
    low = lane < 64
    freq = freq_ref[...]
    lens = len_ref[...].astype(jnp.float32)
    angle = jnp.where(low, to_col(lens[0:1, :]), to_col(lens[1:2, :])) * freq
    cos_p = jnp.cos(angle)
    sin_p = jnp.sin(angle)
    cos_r = pltpu.roll(cos_p, 64, 1)
    sin_r = pltpu.roll(sin_p, 64, 1)
    cos_0 = (jnp.where(low, cos_p, cos_r), jnp.where(low, cos_r, cos_p))
    sin_0 = (jnp.where(low, sin_p, sin_r), jnp.where(low, sin_r, sin_p))

    for i in range(1, 8):
        exchange(i).wait()
    total = parts[0]
    for i in range(1, 8):
        total = total + parts[i]
    q_fac = rms_factor(total[0:n_blk], q_width)
    k_fac = rms_factor(total[n_blk:2 * n_blk], kv_width)
    gain_q = gq_ref[...].astype(jnp.float32)
    gain_k = gk_ref[...].astype(jnp.float32)

    for blk in range(n_blk):
        t, half = blk // 2, blk % 2
        if t == 0:
            cos_t, sin_t = cos_0[half], sin_0[half]
        else:
            cos_s, sin_s = jnp.cos(freq * float(t)), jnp.sin(freq * float(t))
            cos_t = cos_0[half] * cos_s - sin_0[half] * sin_s
            sin_t = sin_0[half] * cos_s + cos_0[half] * sin_s
        sin_t = jnp.where(low, -sin_t, sin_t)

        def rope(val):
            return rounded(val * cos_t + pltpu.roll(val, 64, 1) * sin_t)

        fac = to_col(q_fac[blk:blk + 1, :])
        for g in range(n_heads):
            q_ref[pl.ds(half * 2048 + t * n_heads + g, 128, stride=16), :] = rope(raw[blk, g] * fac * gain_q[:, g * hd:(g + 1) * hd])
        fac = to_col(k_fac[blk:blk + 1, :])
        kv_ref[pl.ds(half * 1024 + t, 128, stride=8), :] = rope(raw[blk, n_heads] * fac * gain_k)


def head_layer(x_seq, cache_len, w_q, w_k, w_v, g_q, g_k, q_width, kv_width, axis):
    n_steps, n_seq, d_model = x_seq.shape
    hd = w_k.shape[1]
    cols = w_q.shape[1] + 2 * hd
    half_dim = hd // 2
    bf16, f32 = jnp.bfloat16, jnp.float32
    inv_freq = ROPE_THETA ** (-(jnp.arange(half_dim, dtype=f32) * (2.0 / hd)))
    freq = jnp.concatenate([inv_freq, inv_freq]).reshape(1, hd)
    anym = pl.BlockSpec(memory_space=pl.ANY)
    vmem = pl.BlockSpec(memory_space=pltpu.VMEM)
    dma = pltpu.SemaphoreType.DMA
    return pl.pallas_call(
        functools.partial(head_kernel, axis, q_width, kv_width),
        out_shape=(jax.ShapeDtypeStruct((n_seq * 16, hd), f32), jax.ShapeDtypeStruct((n_seq * 8, hd), f32)),
        in_specs=[anym] * 4 + [vmem] * 4,
        out_specs=(vmem, vmem),
        scratch_shapes=[
            pltpu.VMEM((n_steps, n_seq, d_model), bf16),
            pltpu.VMEM((d_model, cols), bf16),
            pltpu.VMEM((n_steps, n_seq, cols), f32),
            pltpu.VMEM((2 * n_steps, w_q.shape[1] // hd + 1, 128, hd), f32),
            pltpu.VMEM((16, 128), f32),
            pltpu.VMEM((8, 16, 128), f32),
            dma((N_KB, 4)), dma((7,)), dma((7,)),
        ],
        compiler_params=pltpu.CompilerParams(collective_id=0, has_side_effects=True, vmem_limit_bytes=48 * MIB),
    )(x_seq, w_q, w_k, w_v, g_q.reshape(1, -1), g_k.reshape(1, -1), cache_len.reshape(2, n_seq // 2), freq)


SEQ_BLK = 16
SEQ_GRP = 8


def attn_kernel(n_heads, n_steps, len_ref, q_ref, kv_ref, k_ref, v_ref, o_ref, ko_ref, vo_ref):
    n_pos, hd = k_ref.shape[1:]
    fixed = n_pos // 2
    scale = hd ** -0.5
    base = pl.program_id(0) * SEQ_BLK
    row = lax.broadcasted_iota(jnp.int32, (n_pos - fixed, hd), 0)
    s_step = lax.broadcasted_iota(jnp.int32, (16, n_pos - fixed), 0) // n_heads
    s_last = lax.broadcasted_iota(jnp.int32, (16, n_pos - fixed), 1) + fixed - s_step

    def group(grp, _):
        first = grp * SEQ_GRP
        idx = [first + i for i in range(SEQ_GRP)]
        lens = [len_ref[base + i] for i in idx]
        for i, length in zip(idx, lens):
            rel = row - (length - fixed)
            for in_ref, out_ref, slot in ((k_ref, ko_ref, 0), (v_ref, vo_ref, n_steps)):
                out_ref[i, 0:fixed, :] = in_ref[i, 0:fixed, :]
                vals = in_ref[i, fixed:n_pos, :].astype(jnp.float32)
                for t in range(n_steps):
                    vals = jnp.where(rel == t, kv_ref[i, slot + t:slot + t + 1, :], vals)
                out_ref[i, fixed:n_pos, :] = vals.astype(jnp.bfloat16)
        scores = [lax.dot_general(q_ref[i].astype(jnp.bfloat16), ko_ref[i], (((1,), (1,)), ((), ())), preferred_element_type=jnp.float32) for i in idx]
        probs = []
        sums = []
        for s, length in zip(scores, lens):
            lo = s[:, 0:fixed] * scale
            hi = jnp.where(s_last <= length, s[:, fixed:n_pos] * scale, -jnp.inf)
            top = jnp.max(jnp.maximum(lo, hi), axis=-1, keepdims=True)
            lo = jnp.exp(lo - top)
            hi = jnp.exp(hi - top)
            sums.append(jnp.sum(lo + hi, axis=-1, keepdims=True))
            probs.append(jnp.concatenate([lo.astype(jnp.bfloat16), hi.astype(jnp.bfloat16)], axis=-1))
        for i, p, total in zip(idx, probs, sums):
            o_ref[i] = jnp.dot(p, vo_ref[i], preferred_element_type=jnp.float32) / total
        return 0

    lax.fori_loop(0, SEQ_BLK // SEQ_GRP, group, 0)


def attn_layer(cache_len, q, kv, k_cache, v_cache, n_heads, n_steps):
    n_seq, _, n_pos, hd = k_cache.shape
    bf16, f32 = jnp.bfloat16, jnp.float32
    cache_blk = pl.BlockSpec((SEQ_BLK, n_pos, hd), lambda i: (i, 0, 0))
    o, k_out, v_out = pl.pallas_call(
        functools.partial(attn_kernel, n_heads, n_steps),
        grid=(n_seq // SEQ_BLK,),
        out_shape=(jax.ShapeDtypeStruct((n_seq, 16, hd), f32), jax.ShapeDtypeStruct((n_seq, n_pos, hd), bf16), jax.ShapeDtypeStruct((n_seq, n_pos, hd), bf16)),
        in_specs=[pl.BlockSpec(memory_space=pltpu.SMEM), pl.BlockSpec((SEQ_BLK, 16, hd), lambda i: (i, 0, 0)), pl.BlockSpec((SEQ_BLK, 8, hd), lambda i: (i, 0, 0)), cache_blk, cache_blk],
        out_specs=(pl.BlockSpec((SEQ_BLK, 16, hd), lambda i: (i, 0, 0)), cache_blk, cache_blk),
        compiler_params=pltpu.CompilerParams(vmem_limit_bytes=48 * MIB),
    )(cache_len, q.reshape(n_seq, 16, hd), kv.reshape(n_seq, 8, hd), k_cache.reshape(n_seq, n_pos, hd), v_cache.reshape(n_seq, n_pos, hd))
    return o, k_out.reshape(k_cache.shape), v_out.reshape(v_cache.shape)


N_CB = 4
N_WB = 4
N_DB = 3
HB = 128
DB = 256


def tail_kernel(axis, o_hbm, x_hbm, wo_hbm, w1_hbm, w3_hbm, w2_hbm, ga_ref, gm_ref, y_hbm,
                on, ob, xp, hb, src, recv0, recv1, recv2, act, wob, wb, w2b,
                o_sem, x_sem, wo_sem, wb_sem, w2_sem, y_sem, s_sem, r_sem, g_ssem, g_rsem):
    n_steps, n_seq, d_model = x_hbm.shape
    half = n_seq // 2
    rows = n_steps * half
    piece = rows // 8
    cw = d_model // N_CB
    n_hid = w1_hbm.shape[1]
    n_j = n_hid // HB
    n_d = d_model // DB
    per_cb = n_d // N_CB

    me = lax.axis_index(axis)
    core = lax.rem(me, 2)
    xb = lax.rem(me // 2, 2)
    yb = me // 4
    first_bit = core * yb + (1 - core) * xb
    second_bit = core * xb + (1 - core) * yb
    fw = 1 + core
    sw = 2 - core
    partner = me + 1 - 2 * core
    fpeer = me + (1 - 2 * first_bit) * 2 * fw
    speer = me + (1 - 2 * second_bit) * 2 * sw
    fspeer = fpeer + speer - me

    def remote(src_ref, dst_ref, send, recv, dev):
        return pltpu.make_async_remote_copy(src_ref=src_ref, dst_ref=dst_ref, send_sem=send, recv_sem=recv, device_id={axis: dev}, device_id_type=MESH_ID)

    o_copy = pltpu.make_async_copy(o_hbm, on, o_sem)
    o_copy.start()

    def wo_copy(cb):
        return pltpu.make_async_copy(wo_hbm.at[:, pl.ds(cb * cw, cw)], wob.at[:, pl.ds(cb * cw, cw)], wo_sem.at[cb])

    for cb in range(N_CB):
        wo_copy(cb).start()

    def x_copy(c, i):
        r0 = piece * me + 16 * i
        t = r0 // half
        b = pl.multiple_of(lax.rem(r0, half), 16)
        return pltpu.make_async_copy(x_hbm.at[t, pl.ds(c * half + b, 16), :], xp.at[c, pl.ds(16 * i, 16), :], x_sem.at[c, i])

    for c in range(2):
        for i in range(piece // 16):
            x_copy(c, i).start()

    def wb_copies(j, s):
        col = pl.ds(pl.multiple_of(j * HB, HB), HB)
        return (pltpu.make_async_copy(w1_hbm.at[:, col], wb.at[s, :, 0:HB], wb_sem.at[s, 0]),
                pltpu.make_async_copy(w3_hbm.at[:, col], wb.at[s, :, HB:2 * HB], wb_sem.at[s, 1]))

    def w2_copy(j, s):
        return pltpu.make_async_copy(w2_hbm.at[:, pl.ds(pl.multiple_of(j * DB, DB), DB)], w2b.at[s], w2_sem.at[s])

    for s in range(N_WB - 1):
        for cp in wb_copies(s, s):
            cp.start()

    bar = pltpu.get_barrier_semaphore()
    for dev in (partner, fpeer, speer):
        pl.semaphore_signal(bar, inc=1, device_id={axis: dev}, device_id_type=MESH_ID)
    pl.semaphore_wait(bar, 3)

    def cols_of(cb):
        return pl.ds(pl.multiple_of(cb * cw, cw), cw)

    def copy0(inst, cb):
        c = inst % 2
        return remote(src.at[c, :, 1 - core, :, cols_of(cb)], recv0.at[c, :, :, cols_of(cb)], s_sem.at[inst, 0, cb], r_sem.at[inst, 0, cb], partner)

    def copy1(inst, cb, k):
        c = inst % 2
        sb = (1 - second_bit) if k == 0 else second_bit
        idx = (1 - first_bit) * fw + sb * sw
        return remote(recv0.at[c, idx, :, cols_of(cb)], recv1.at[c, k, :, cols_of(cb)], s_sem.at[inst, 1 + k, cb], r_sem.at[inst, 1 + k, cb], fpeer)

    def copy2(inst, cb):
        c = inst % 2
        return remote(recv1.at[c, 0, :, cols_of(cb)], recv2.at[c, :, cols_of(cb)], s_sem.at[inst, 3, cb], r_sem.at[inst, 3, cb], speer)

    def f32(v):
        return v.astype(jnp.float32)

    def event1(inst, cb):
        c = inst % 2
        copy0(inst, cb).wait_recv()
        cols = cols_of(cb)

        def add(i, _):
            recv0[c, i, :, cols] = (f32(src[c, i, core, :, cols]) + f32(recv0[c, i, :, cols])).astype(jnp.bfloat16)
            return 0

        lax.fori_loop(0, 4, add, 0)
        copy1(inst, cb, 0).start()
        copy1(inst, cb, 1).start()

    def event2(inst, cb):
        c = inst % 2
        copy1(inst, cb, 0).wait_recv()
        cols = cols_of(cb)
        idx = first_bit * fw + (1 - second_bit) * sw
        recv1[c, 0, :, cols] = (f32(recv0[c, idx, :, cols]) + f32(recv1[c, 0, :, cols])).astype(jnp.bfloat16)
        copy2(inst, cb).start()

    def event3(inst, cb):
        c = inst % 2
        copy1(inst, cb, 1).wait_recv()
        copy2(inst, cb).wait_recv()
        cols = cols_of(cb)
        idx = first_bit * fw + second_bit * sw
        recv2[c, :, cols] = (f32(recv0[c, idx, :, cols]) + f32(recv1[c, 1, :, cols]) + f32(recv2[c, :, cols])).astype(jnp.bfloat16)

    def rows_of(c, dev):
        return hb.at[c, pl.ds(pl.multiple_of(dev * piece, 16), piece), :]

    def gcopy(inst, k):
        c = inst % 2
        who, dev = ((me, speer), (me, fpeer), (me, partner), (speer, fpeer), (speer, partner), (fpeer, partner), (fspeer, partner))[k]
        return remote(rows_of(c, who), rows_of(c, who), g_ssem.at[inst, k], g_rsem.at[inst, k], dev)

    def event4(inst):
        c = inst % 2
        gain_ref = ga_ref if inst < 2 else gm_ref

        def one(i, _):
            r = pl.ds(pl.multiple_of(i * 16, 16), 16)
            hr = pl.ds(pl.multiple_of(me * piece + i * 16, 16), 16)
            a = f32(recv2[c, r, :])
            factor = rms_factor(jnp.sum(a * a, axis=-1, keepdims=True), d_model)
            base = f32(xp[c, r, :]) if inst < 2 else f32(hb[c, hr, :])
            hb[c, hr, :] = (base + a * factor * f32(gain_ref[...])).astype(jnp.bfloat16)
            return 0

        lax.fori_loop(0, piece // 16, one, 0)

        def drain(cb, _):
            copy0(inst, cb).wait_send()
            copy1(inst, cb, 0).wait_send()
            copy1(inst, cb, 1).wait_send()
            copy2(inst, cb).wait_send()
            return 0

        lax.fori_loop(0, N_CB, drain, 0)
        for k in (1, 0, 2):
            gcopy(inst, k).start()

    def event5(inst):
        gcopy(inst, 0).wait_recv()
        gcopy(inst, 3).start()
        gcopy(inst, 4).start()

    def event6(inst):
        gcopy(inst, 1).wait_recv()
        gcopy(inst, 5).start()

    def event7(inst):
        gcopy(inst, 3).wait_recv()
        gcopy(inst, 6).start()

    def event8(inst):
        for k in (2, 4, 5, 6):
            gcopy(inst, k).wait_recv()
        for k in range(7):
            gcopy(inst, k).wait_send()

    def span(j, start, every, fn):
        k = j - start

        @pl.when((k >= 0) & (k < every * N_CB) & (lax.rem(k + every, every) == 0))
        def _():
            fn(k // every)

    def at(j, when, fn):
        @pl.when(j == when)
        def _():
            fn()

    hd = o_hbm.shape[1]
    n_heads = wo_hbm.shape[0] // hd

    def out_proj(c):
        for t in range(n_steps):
            for g in range(n_heads):
                ob[c, t * half:(t + 1) * half, g * hd:(g + 1) * hd] = on[pl.ds(c * half * 16 + t * n_heads + g, half, stride=16), :].astype(jnp.bfloat16)

        def step(cb, _):
            part = jnp.dot(ob[c], wob[:, cols_of(cb)], preferred_element_type=jnp.float32).astype(jnp.bfloat16)
            src[c, :, :, :, cols_of(cb)] = part.reshape(4, 2, piece, cw)
            copy0(c, cb).start()
            return 0

        lax.fori_loop(0, N_CB, step, 0)

    def y_copies(c):
        return [pltpu.make_async_copy(hb.at[c, pl.ds(t * half, half), :], y_hbm.at[t, pl.ds(c * half, half), :], y_sem.at[c, t]) for t in range(n_steps)]

    o_copy.wait()
    for cb in range(N_CB):
        wo_copy(cb).wait()
    out_proj(0)
    lax.fori_loop(0, N_CB, lambda cb, _: (event1(0, cb), 0)[1], 0)
    out_proj(1)
    for c in range(2):
        for i in range(piece // 16):
            x_copy(c, i).wait()
    lax.fori_loop(0, N_CB, lambda cb, _: (event2(0, cb), 0)[1], 0)
    lax.fori_loop(0, N_CB, lambda cb, _: (event3(0, cb), 0)[1], 0)
    event4(0)
    event5(0)
    event6(0)
    event7(0)
    event8(0)

    for c in range(2):
        other = 1 + c

        def gate_up(j, _):
            s = lax.rem(j, N_WB)

            @pl.when(j + N_WB - 1 < n_j)
            def _():
                for cp in wb_copies(j + N_WB - 1, lax.rem(j + N_WB - 1, N_WB)):
                    cp.start()

            for cp in wb_copies(j, s):
                cp.wait()
            both = jnp.dot(hb[c], wb[s], preferred_element_type=jnp.float32)
            gate = both[:, :HB]
            act[:, pl.ds(pl.multiple_of(j * HB, HB), HB)] = (jax.nn.silu(gate) * both[:, HB:]).astype(jnp.bfloat16)
            span(j, 1, 1, functools.partial(event1, other))
            span(j, 6, 2, functools.partial(event2, other))
            span(j, 10, 2, functools.partial(event3, other))
            at(j, 17, functools.partial(event4, other))
            at(j, 24, functools.partial(event5, other))
            at(j, 25, functools.partial(event6, other))
            return 0

        for s in range(N_DB - 1):
            w2_copy(s, s).start()
        lax.fori_loop(0, n_j, gate_up, 0)
        if c == 0:
            for s in range(N_WB - 1):
                for cp in wb_copies(s, s):
                    cp.start()

        def down(j, _):
            s = lax.rem(j, N_DB)

            @pl.when(j + N_DB - 1 < n_d)
            def _():
                w2_copy(j + N_DB - 1, lax.rem(j + N_DB - 1, N_DB)).start()

            w2_copy(j, s).wait()
            part = jnp.dot(act[...], w2b[s], preferred_element_type=jnp.float32).astype(jnp.bfloat16)
            src[c, :, :, :, pl.ds(pl.multiple_of(j * DB, DB), DB)] = part.reshape(4, 2, piece, DB)

            @pl.when(lax.rem(j, per_cb) == per_cb - 1)
            def _():
                copy0(2 + c, j // per_cb).start()

            at(j, 7, functools.partial(event7, other))
            at(j, 10, functools.partial(event8, other))
            if c == 1:
                q = j // per_cb

                @pl.when(lax.rem(j, per_cb) == 2)
                def _():
                    @pl.when(q >= 1)
                    def _():
                        event1(3, q - 1)

                    @pl.when(q >= 2)
                    def _():
                        event2(3, q - 2)

                    @pl.when(q >= 3)
                    def _():
                        event3(3, q - 3)
            return 0

        lax.fori_loop(0, n_d, down, 0)
        if c == 1:
            for cp in y_copies(0):
                cp.start()

    event1(3, 3)
    event2(3, 2)
    event3(3, 1)
    event2(3, 3)
    event3(3, 2)
    event3(3, 3)
    event4(3)
    event5(3)
    event6(3)
    event7(3)
    event8(3)
    for cp in y_copies(1):
        cp.start()
    for c in range(2):
        for cp in y_copies(c):
            cp.wait()


def tail_layer(o, x_seq, w_o, w_gate, w_up, w_down, g_attn, g_mlp, axis):
    n_steps, n_seq, d_model = x_seq.shape
    rows = n_steps * n_seq // 2
    piece = rows // 8
    n_hid = w_gate.shape[1]
    bf16 = jnp.bfloat16
    anym = pl.BlockSpec(memory_space=pl.ANY)
    vmem = pl.BlockSpec(memory_space=pltpu.VMEM)
    dma = pltpu.SemaphoreType.DMA
    return pl.pallas_call(
        functools.partial(tail_kernel, axis),
        out_shape=jax.ShapeDtypeStruct((n_steps, n_seq, d_model), bf16),
        in_specs=[anym] * 6 + [vmem] * 2,
        out_specs=anym,
        scratch_shapes=[
            pltpu.VMEM(o.shape, jnp.float32),
            pltpu.VMEM((2, rows, w_o.shape[0]), bf16),
            pltpu.VMEM((2, piece, d_model), bf16),
            pltpu.VMEM((2, rows, d_model), bf16),
            pltpu.VMEM((2, 4, 2, piece, d_model), bf16),
            pltpu.VMEM((2, 4, piece, d_model), bf16),
            pltpu.VMEM((2, 2, piece, d_model), bf16),
            pltpu.VMEM((2, piece, d_model), bf16),
            pltpu.VMEM((rows, n_hid), bf16),
            pltpu.VMEM(w_o.shape, bf16),
            pltpu.VMEM((N_WB, d_model, 2 * HB), bf16),
            pltpu.VMEM((N_DB, n_hid, DB), bf16),
            dma, dma((2, piece // 16)), dma((N_CB,)), dma((N_WB, 2)), dma((N_DB,)), dma((2, n_steps)),
            dma((4, 4, N_CB)), dma((4, 4, N_CB)), dma((4, 7)), dma((4, 7)),
        ],
        compiler_params=pltpu.CompilerParams(collective_id=1, has_side_effects=True, vmem_limit_bytes=63 * MIB),
    )(o, x_seq, w_o, w_gate, w_up, w_down, g_attn.reshape(1, -1), g_mlp.reshape(1, -1))


def layer_steps(x_seq, cache_len, k_cache, v_cache, w_q, w_k, w_v, w_o, w_gate, w_up, w_down, g_q, g_k, g_attn, g_mlp, q_width, kv_width):
    n_steps, n_seq, _ = x_seq.shape
    hd = k_cache.shape[-1]
    q, kv = head_layer(x_seq, cache_len, w_q, w_k, w_v, g_q, g_k, q_width, kv_width, 'tp')
    o, k_out, v_out = attn_layer(cache_len, q, kv, k_cache, v_cache, w_q.shape[1] // hd, n_steps)
    y = tail_layer(o.reshape(n_seq * 16, hd), x_seq, w_o, w_gate, w_up, w_down, g_attn, g_mlp, 'tp')
    return y, k_out, v_out


def solution(mesh):
    tp_size = mesh.shape['tp']

    def local_run(x_seq, cache_len, k_cache, v_cache, w_q, w_k, w_v, w_o, w_gate, w_up, w_down, g_q, g_k, g_attn, g_mlp):
        return layer_steps(x_seq, cache_len, k_cache, v_cache, w_q, w_k, w_v, w_o, w_gate, w_up, w_down, g_q, g_k, g_attn, g_mlp, w_q.shape[1] * tp_size, w_k.shape[1] * tp_size)

    data_spec = P(None, 'dp', None)
    cache_spec = P('dp', 'tp', None, None)
    col_spec = P(None, 'tp')
    row_spec = P('tp', None)
    arg_specs = (data_spec, P('dp'), cache_spec, cache_spec, col_spec, col_spec, col_spec, row_spec, col_spec, col_spec, row_spec, P('tp'), P('tp'), P(None), P(None))
    out_specs = (data_spec, cache_spec, cache_spec)
    return jax.shard_map(local_run, mesh=mesh, in_specs=arg_specs, out_specs=out_specs, check_vma=False)
```

```python
import functools

import jax
import jax.numpy as jnp
from jax import lax
from jax.experimental import pallas as pl
from jax.experimental.pallas import tpu as pltpu
from jax.sharding import PartitionSpec as P

ROPE_THETA = 500000.0
NORM_EPS = 1e-6
MESH_ID = pl.DeviceIdType.MESH
MIB = 2**20


def rms_factor(sq_sum, full_width):
    return lax.rsqrt(sq_sum / full_width + NORM_EPS)


N_KB = 5


def head_kernel(axis, q_width, kv_width, x_hbm, wq_hbm, wk_hbm, wv_hbm, gq_ref, gk_ref, len_ref, freq_ref, q_ref, kv_ref,
                xv, wv, acc, raw, sums, parts, in_sem, s_sem, r_sem):
    n_steps, n_seq, d_model = x_hbm.shape
    wq_cols = wq_hbm.shape[1]
    hd = wk_hbm.shape[1]
    n_heads = wq_cols // hd
    kw = d_model // N_KB
    n_blk = n_steps * 2
    me = lax.axis_index(axis)

    def in_copies(kb):
        ks = pl.ds(pl.multiple_of(kb * kw, kw), kw)
        return (pltpu.make_async_copy(x_hbm.at[:, :, ks], xv.at[:, :, ks], in_sem.at[kb, 0]),
                pltpu.make_async_copy(wq_hbm.at[ks, :], wv.at[ks, 0:wq_cols], in_sem.at[kb, 1]),
                pltpu.make_async_copy(wk_hbm.at[ks, :], wv.at[ks, wq_cols:wq_cols + hd], in_sem.at[kb, 2]),
                pltpu.make_async_copy(wv_hbm.at[ks, :], wv.at[ks, wq_cols + hd:wq_cols + 2 * hd], in_sem.at[kb, 3]))

    for kb in range(N_KB):
        for cp in in_copies(kb):
            cp.start()

    bar = pltpu.get_barrier_semaphore()
    for i in range(1, 8):
        pl.semaphore_signal(bar, inc=1, device_id={axis: lax.rem(me + i, 8)}, device_id_type=MESH_ID)

    def project(kb, _):
        for cp in in_copies(kb):
            cp.wait()
        ks = pl.ds(pl.multiple_of(kb * kw, kw), kw)
        for t in range(n_steps):
            part = jnp.dot(xv[t, :, ks], wv[ks, :], preferred_element_type=jnp.float32)

            @pl.when(kb == 0)
            def _():
                acc[t] = part

            @pl.when(kb > 0)
            def _():
                acc[t] += part
        return 0

    lax.fori_loop(0, N_KB, project, 0)

    lane = lax.broadcasted_iota(jnp.int32, (128, 128), 1)
    diag = lane == lax.broadcasted_iota(jnp.int32, (128, 128), 0)

    def to_row(col):
        return jnp.sum(jnp.where(diag, jnp.broadcast_to(col, (128, 128)), 0.0), axis=0, keepdims=True)

    def to_col(row):
        return jnp.sum(jnp.where(diag, jnp.broadcast_to(row, (128, 128)), 0.0), axis=1, keepdims=True)

    def rounded(v):
        return v.astype(jnp.bfloat16).astype(jnp.float32)

    sums[...] = jnp.zeros_like(sums)
    for blk in range(n_blk):
        t, half = blk // 2, blk % 2
        rows = slice(half * 128, half * 128 + 128)
        sq = None
        for g in range(n_heads):
            val = rounded(acc[t, rows, g * hd:(g + 1) * hd])
            raw[blk, g] = val
            sq = val * val if sq is None else sq + val * val
        sums[blk:blk + 1, :] = to_row(jnp.sum(sq, axis=-1, keepdims=True))
        val = rounded(acc[t, rows, wq_cols:wq_cols + hd])
        raw[blk, n_heads] = val
        sums[n_blk + blk:n_blk + blk + 1, :] = to_row(jnp.sum(val * val, axis=-1, keepdims=True))

    def exchange(i):
        return pltpu.make_async_remote_copy(src_ref=sums, dst_ref=parts.at[me], send_sem=s_sem.at[i - 1], recv_sem=r_sem.at[i - 1], device_id={axis: lax.rem(me + i, 8)}, device_id_type=MESH_ID)

    pl.semaphore_wait(bar, 7)
    for i in range(1, 8):
        exchange(i).start()
    parts[me] = sums[...]

    for blk in range(n_blk):
        t, half = blk // 2, blk % 2
        rows = slice(half * 128, half * 128 + 128)
        kv_ref[pl.ds(half * 1024 + 3 + t, 128, stride=8), :] = rounded(acc[t, rows, wq_cols + hd:wq_cols + 2 * hd])
    for half in range(2):
        zero = jnp.zeros((128, hd), jnp.float32)
        for slot in range(n_steps * n_heads, 16):
            q_ref[pl.ds(half * 2048 + slot, 128, stride=16), :] = zero
        for slot in range(2 * n_steps, 8):
            kv_ref[pl.ds(half * 1024 + slot, 128, stride=8), :] = zero
    low = lane < 64
    freq = freq_ref[...]
    lens = len_ref[...].astype(jnp.float32)
    angle = jnp.where(low, to_col(lens[0:1, :]), to_col(lens[1:2, :])) * freq
    cos_p = jnp.cos(angle)
    sin_p = jnp.sin(angle)
    cos_r = pltpu.roll(cos_p, 64, 1)
    sin_r = pltpu.roll(sin_p, 64, 1)
    cos_0 = (jnp.where(low, cos_p, cos_r), jnp.where(low, cos_r, cos_p))
    sin_0 = (jnp.where(low, sin_p, sin_r), jnp.where(low, sin_r, sin_p))

    for i in range(1, 8):
        exchange(i).wait()
    total = parts[0]
    for i in range(1, 8):
        total = total + parts[i]
    q_fac = rms_factor(total[0:n_blk], q_width)
    k_fac = rms_factor(total[n_blk:2 * n_blk], kv_width)
    gain_q = gq_ref[...].astype(jnp.float32)
    gain_k = gk_ref[...].astype(jnp.float32)

    for blk in range(n_blk):
        t, half = blk // 2, blk % 2
        if t == 0:
            cos_t, sin_t = cos_0[half], sin_0[half]
        else:
            cos_s, sin_s = jnp.cos(freq * float(t)), jnp.sin(freq * float(t))
            cos_t = cos_0[half] * cos_s - sin_0[half] * sin_s
            sin_t = sin_0[half] * cos_s + cos_0[half] * sin_s
        sin_t = jnp.where(low, -sin_t, sin_t)

        def rope(val):
            return rounded(val * cos_t + pltpu.roll(val, 64, 1) * sin_t)

        fac = to_col(q_fac[blk:blk + 1, :])
        for g in range(n_heads):
            q_ref[pl.ds(half * 2048 + t * n_heads + g, 128, stride=16), :] = rope(raw[blk, g] * fac * gain_q[:, g * hd:(g + 1) * hd])
        fac = to_col(k_fac[blk:blk + 1, :])
        kv_ref[pl.ds(half * 1024 + t, 128, stride=8), :] = rope(raw[blk, n_heads] * fac * gain_k)


def head_layer(x_seq, cache_len, w_q, w_k, w_v, g_q, g_k, q_width, kv_width, axis):
    n_steps, n_seq, d_model = x_seq.shape
    hd = w_k.shape[1]
    cols = w_q.shape[1] + 2 * hd
    half_dim = hd // 2
    bf16, f32 = jnp.bfloat16, jnp.float32
    inv_freq = ROPE_THETA ** (-(jnp.arange(half_dim, dtype=f32) * (2.0 / hd)))
    freq = jnp.concatenate([inv_freq, inv_freq]).reshape(1, hd)
    anym = pl.BlockSpec(memory_space=pl.ANY)
    vmem = pl.BlockSpec(memory_space=pltpu.VMEM)
    dma = pltpu.SemaphoreType.DMA
    return pl.pallas_call(
        functools.partial(head_kernel, axis, q_width, kv_width),
        out_shape=(jax.ShapeDtypeStruct((n_seq * 16, hd), f32), jax.ShapeDtypeStruct((n_seq * 8, hd), f32)),
        in_specs=[anym] * 4 + [vmem] * 4,
        out_specs=(vmem, vmem),
        scratch_shapes=[
            pltpu.VMEM((n_steps, n_seq, d_model), bf16),
            pltpu.VMEM((d_model, cols), bf16),
            pltpu.VMEM((n_steps, n_seq, cols), f32),
            pltpu.VMEM((2 * n_steps, w_q.shape[1] // hd + 1, 128, hd), f32),
            pltpu.VMEM((16, 128), f32),
            pltpu.VMEM((8, 16, 128), f32),
            dma((N_KB, 4)), dma((7,)), dma((7,)),
        ],
        compiler_params=pltpu.CompilerParams(collective_id=0, has_side_effects=True, vmem_limit_bytes=48 * MIB),
    )(x_seq, w_q, w_k, w_v, g_q.reshape(1, -1), g_k.reshape(1, -1), cache_len.reshape(2, n_seq // 2), freq)


SEQ_BLK = 16
SEQ_GRP = 8


def attn_kernel(n_heads, n_steps, len_ref, q_ref, kv_ref, k_ref, v_ref, o_ref, ko_ref, vo_ref):
    n_pos, hd = k_ref.shape[1:]
    fixed = n_pos // 2
    scale = hd ** -0.5
    base = pl.program_id(0) * SEQ_BLK
    row = lax.broadcasted_iota(jnp.int32, (n_pos - fixed, hd), 0)
    s_step = lax.broadcasted_iota(jnp.int32, (16, n_pos - fixed), 0) // n_heads
    s_last = lax.broadcasted_iota(jnp.int32, (16, n_pos - fixed), 1) + fixed - s_step

    def group(grp, _):
        first = grp * SEQ_GRP
        idx = [first + i for i in range(SEQ_GRP)]
        lens = [len_ref[base + i] for i in idx]
        for i, length in zip(idx, lens):
            rel = row - (length - fixed)
            for in_ref, out_ref, slot in ((k_ref, ko_ref, 0), (v_ref, vo_ref, n_steps)):
                out_ref[i, 0:fixed, :] = in_ref[i, 0:fixed, :]
                vals = in_ref[i, fixed:n_pos, :].astype(jnp.float32)
                for t in range(n_steps):
                    vals = jnp.where(rel == t, kv_ref[i, slot + t:slot + t + 1, :], vals)
                out_ref[i, fixed:n_pos, :] = vals.astype(jnp.bfloat16)
        scores = [lax.dot_general(q_ref[i].astype(jnp.bfloat16), ko_ref[i], (((1,), (1,)), ((), ())), preferred_element_type=jnp.float32) for i in idx]
        probs = []
        sums = []
        for s, length in zip(scores, lens):
            lo = s[:, 0:fixed] * scale
            hi = jnp.where(s_last <= length, s[:, fixed:n_pos] * scale, -jnp.inf)
            top = jnp.max(jnp.maximum(lo, hi), axis=-1, keepdims=True)
            lo = jnp.exp(lo - top)
            hi = jnp.exp(hi - top)
            sums.append(jnp.sum(lo + hi, axis=-1, keepdims=True))
            probs.append(jnp.concatenate([lo.astype(jnp.bfloat16), hi.astype(jnp.bfloat16)], axis=-1))
        for i, p, total in zip(idx, probs, sums):
            o_ref[i] = jnp.dot(p, vo_ref[i], preferred_element_type=jnp.float32) / total
        return 0

    lax.fori_loop(0, SEQ_BLK // SEQ_GRP, group, 0)


def attn_layer(cache_len, q, kv, k_cache, v_cache, n_heads, n_steps):
    n_seq, _, n_pos, hd = k_cache.shape
    bf16, f32 = jnp.bfloat16, jnp.float32
    cache_blk = pl.BlockSpec((SEQ_BLK, n_pos, hd), lambda i: (i, 0, 0))
    o, k_out, v_out = pl.pallas_call(
        functools.partial(attn_kernel, n_heads, n_steps),
        grid=(n_seq // SEQ_BLK,),
        out_shape=(jax.ShapeDtypeStruct((n_seq, 16, hd), f32), jax.ShapeDtypeStruct((n_seq, n_pos, hd), bf16), jax.ShapeDtypeStruct((n_seq, n_pos, hd), bf16)),
        in_specs=[pl.BlockSpec(memory_space=pltpu.SMEM), pl.BlockSpec((SEQ_BLK, 16, hd), lambda i: (i, 0, 0)), pl.BlockSpec((SEQ_BLK, 8, hd), lambda i: (i, 0, 0)), cache_blk, cache_blk],
        out_specs=(pl.BlockSpec((SEQ_BLK, 16, hd), lambda i: (i, 0, 0)), cache_blk, cache_blk),
        compiler_params=pltpu.CompilerParams(vmem_limit_bytes=48 * MIB),
    )(cache_len, q.reshape(n_seq, 16, hd), kv.reshape(n_seq, 8, hd), k_cache.reshape(n_seq, n_pos, hd), v_cache.reshape(n_seq, n_pos, hd))
    return o, k_out.reshape(k_cache.shape), v_out.reshape(v_cache.shape)


N_CB = 5
N_SUB = 2
N_WB = 4
N_DB = 3
HB = 128
DB = 512


def tail_kernel(axis, o_hbm, x_hbm, wo_hbm, w1_hbm, w3_hbm, w2_hbm, gains_hbm, y_hbm,
                on, ob, xp, hb, src, recv0, recv1, recv2, act, wob, wb, w2b, gains,
                o_sem, x_sem, wo_sem, wb_sem, w2_sem, y_sem, gain_sem, s_sem, r_sem, g_ssem, g_rsem):
    n_steps, n_seq, d_model = x_hbm.shape
    piece = n_seq // 8
    sub_rows = piece // N_SUB
    cw = d_model // N_CB
    n_hid = w1_hbm.shape[1]
    n_j = n_hid // HB
    n_d = d_model // DB
    per_cb = n_d // N_CB
    hd = o_hbm.shape[1]
    n_heads = wo_hbm.shape[0] // hd

    me = lax.axis_index(axis)
    core = lax.rem(me, 2)
    xb = lax.rem(me // 2, 2)
    yb = me // 4
    first_bit = core * yb + (1 - core) * xb
    second_bit = core * xb + (1 - core) * yb
    fw = 1 + core
    sw = 2 - core
    partner = me + 1 - 2 * core
    fpeer = me + (1 - 2 * first_bit) * 2 * fw
    speer = me + (1 - 2 * second_bit) * 2 * sw
    fspeer = fpeer + speer - me

    def remote(src_ref, dst_ref, send, recv, dev):
        return pltpu.make_async_remote_copy(src_ref=src_ref, dst_ref=dst_ref, send_sem=send, recv_sem=recv, device_id={axis: dev}, device_id_type=MESH_ID)

    o_copy = pltpu.make_async_copy(o_hbm, on, o_sem)
    o_copy.start()

    def wo_copy(cb):
        return pltpu.make_async_copy(wo_hbm.at[:, pl.ds(cb * cw, cw)], wob.at[:, pl.ds(cb * cw, cw)], wo_sem.at[cb])

    for cb in range(N_CB):
        wo_copy(cb).start()
    gain_copy = pltpu.make_async_copy(gains_hbm, gains, gain_sem)
    gain_copy.start()
    x_copy = pltpu.make_async_copy(x_hbm.at[:, pl.ds(pl.multiple_of(piece * me, piece), piece), :], xp, x_sem)
    x_copy.start()

    def wb_copies(j, s):
        col = pl.ds(pl.multiple_of(j * HB, HB), HB)
        return (pltpu.make_async_copy(w1_hbm.at[:, col], wb.at[s, :, 0:HB], wb_sem.at[s, 0]),
                pltpu.make_async_copy(w3_hbm.at[:, col], wb.at[s, :, HB:2 * HB], wb_sem.at[s, 1]))

    def w2_copy(j, s):
        return pltpu.make_async_copy(w2_hbm.at[:, pl.ds(pl.multiple_of(j * DB, DB), DB)], w2b.at[s], w2_sem.at[s])

    def start_wb():
        for s in range(N_WB - 1):
            for cp in wb_copies(s, s):
                cp.start()

    start_wb()

    bar = pltpu.get_barrier_semaphore()
    for dev in (partner, fpeer, speer):
        pl.semaphore_signal(bar, inc=1, device_id={axis: dev}, device_id_type=MESH_ID)
    pl.semaphore_wait(bar, 3)

    def cols_of(cb):
        return pl.ds(pl.multiple_of(cb * cw, cw), cw)

    def copy0(inst, cb):
        c = inst % n_steps
        return remote(src.at[c, :, 1 - core, :, cols_of(cb)], recv0.at[c, :, :, cols_of(cb)], s_sem.at[inst, 0, cb], r_sem.at[inst, 0, cb], partner)

    def copy1(inst, cb, k):
        c = inst % n_steps
        sb = (1 - second_bit) if k == 0 else second_bit
        idx = (1 - first_bit) * fw + sb * sw
        return remote(recv0.at[c, idx, :, cols_of(cb)], recv1.at[c, k, :, cols_of(cb)], s_sem.at[inst, 1 + k, cb], r_sem.at[inst, 1 + k, cb], fpeer)

    def copy2(inst, cb):
        c = inst % n_steps
        return remote(recv1.at[c, 0, :, cols_of(cb)], recv2.at[c, :, cols_of(cb)], s_sem.at[inst, 3, cb], r_sem.at[inst, 3, cb], speer)

    def f32(v):
        return v.astype(jnp.float32)

    def event1(inst, cb):
        c = inst % n_steps
        copy0(inst, cb).wait_recv()
        cols = cols_of(cb)

        def add(i, _):
            recv0[c, i, :, cols] = (f32(src[c, i, core, :, cols]) + f32(recv0[c, i, :, cols])).astype(jnp.bfloat16)
            return 0

        lax.fori_loop(0, 4, add, 0)
        copy1(inst, cb, 0).start()
        copy1(inst, cb, 1).start()

    def event2(inst, cb):
        c = inst % n_steps
        copy1(inst, cb, 0).wait_recv()
        cols = cols_of(cb)
        idx = first_bit * fw + (1 - second_bit) * sw
        recv1[c, 0, :, cols] = (f32(recv0[c, idx, :, cols]) + f32(recv1[c, 0, :, cols])).astype(jnp.bfloat16)
        copy2(inst, cb).start()

    def event3(inst, cb):
        c = inst % n_steps
        copy1(inst, cb, 1).wait_recv()
        copy2(inst, cb).wait_recv()
        cols = cols_of(cb)
        idx = first_bit * fw + second_bit * sw
        recv2[c, :, cols] = (f32(recv0[c, idx, :, cols]) + f32(recv1[c, 1, :, cols]) + f32(recv2[c, :, cols])).astype(jnp.bfloat16)

    def gcopy(inst, k, sub):
        c = inst % n_steps
        who, dev = ((me, speer), (me, fpeer), (me, partner), (speer, fpeer), (speer, partner), (fpeer, partner), (fspeer, partner))[k]
        part = hb.at[c, pl.ds(pl.multiple_of(who * piece + sub * sub_rows, sub_rows), sub_rows), :]
        return remote(part, part, g_ssem.at[inst, k, sub], g_rsem.at[inst, k, sub], dev)

    def event4(inst, sub):
        c = inst % n_steps
        attn = inst < n_steps

        @pl.when(sub == 0)
        def _():
            def drain(cb, _):
                copy0(inst, cb).wait_send()
                copy1(inst, cb, 0).wait_send()
                copy1(inst, cb, 1).wait_send()
                copy2(inst, cb).wait_send()
                return 0

            lax.fori_loop(0, N_CB, drain, 0)

        r = pl.ds(pl.multiple_of(sub * sub_rows, sub_rows), sub_rows)
        hr = pl.ds(pl.multiple_of(me * piece + sub * sub_rows, sub_rows), sub_rows)
        a = f32(recv2[c, r, :])
        factor = rms_factor(jnp.sum(a * a, axis=-1, keepdims=True), d_model)
        base = f32(xp[c, r, :]) if attn else f32(hb[c, hr, :])
        gain = gains[0:1, :] if attn else gains[1:2, :]
        hb[c, hr, :] = (base + a * factor * gain).astype(jnp.bfloat16)
        for k in (1, 0, 2):
            gcopy(inst, k, sub).start()

    def event5(inst, sub):
        gcopy(inst, 0, sub).wait_recv()
        gcopy(inst, 3, sub).start()
        gcopy(inst, 4, sub).start()
        gcopy(inst, 1, sub).wait_recv()
        gcopy(inst, 5, sub).start()

    def event7(inst, sub):
        gcopy(inst, 3, sub).wait_recv()
        gcopy(inst, 6, sub).start()

    def event8(inst, sub):
        for k in (2, 4, 5, 6):
            gcopy(inst, k, sub).wait_recv()
        for k in range(7):
            gcopy(inst, k, sub).wait_send()

    def run(j, table):
        for event, inst, start, every, count in table:
            k = j - start
            cond = (k >= 0) & (k < every * count)
            if every > 1:
                cond = cond & (lax.rem(k, every) == 0)

            @pl.when(cond)
            def _():
                event(inst, k // every)

    def loop(n, fn):
        lax.fori_loop(0, n, lambda i, _: (fn(i), 0)[1], 0)

    def out_proj(c):
        for g in range(n_heads):
            ob[:, g * hd:(g + 1) * hd] = on[pl.ds(c * n_heads + g, n_seq, stride=16), :].astype(jnp.bfloat16)

        def step(cb):
            part = jnp.dot(ob[...], wob[:, cols_of(cb)], preferred_element_type=jnp.float32).astype(jnp.bfloat16)
            src[c, :, :, :, cols_of(cb)] = part.reshape(4, 2, piece, cw)
            copy0(c, cb).start()

        loop(N_CB, step)

    def y_copy(c):
        return pltpu.make_async_copy(hb.at[c], y_hbm.at[c], y_sem.at[c])

    o_copy.wait()
    for cb in range(N_CB):
        wo_copy(cb).wait()
    out_proj(0)
    loop(N_CB, functools.partial(event1, 0))
    out_proj(1)
    out_proj(2)
    x_copy.wait()
    gain_copy.wait()

    def finish_reduce(inst):
        def step(k):
            @pl.when(k < N_CB)
            def _():
                event2(inst, k)

            @pl.when(k > 0)
            def _():
                event3(inst, k - 1)

        loop(N_CB + 1, step)

    def finish_gather(inst):
        loop(N_SUB, functools.partial(event4, inst))
        loop(N_SUB, functools.partial(event5, inst))
        loop(N_SUB, functools.partial(event7, inst))
        loop(N_SUB, functools.partial(event8, inst))

    finish_reduce(0)
    finish_gather(0)

    gate_tables = (
        ((event1, 1, 0, 1, N_CB), (event2, 1, 4, 2, N_CB), (event3, 1, 9, 2, N_CB), (event4, 1, 18, 1, N_SUB), (event1, 2, 20, 1, N_CB)),
        ((event1, 3, 0, 1, N_CB), (event2, 3, 6, 3, N_CB), (event5, 2, 10, 1, N_SUB), (event3, 3, 10, 3, N_CB), (event7, 2, 17, 1, N_SUB), (event8, 2, 20, 1, N_SUB), (event4, 3, 24, 1, N_SUB)),
        ((event1, 4, 0, 1, N_CB), (event7, 3, 2, 1, N_SUB), (event2, 4, 6, 2, N_CB), (event8, 3, 7, 1, N_SUB), (event3, 4, 10, 2, N_CB), (event4, 4, 19, 1, N_SUB)),
    )
    down_tables = (
        ((event2, 2, 0, 1, N_CB), (event3, 2, 4, 1, N_CB), (event5, 1, 3, 1, N_SUB), (event7, 1, 7, 1, N_SUB), (event8, 1, 9, 1, 1)),
        ((event5, 3, 6, 1, N_SUB),),
        ((event5, 4, 3, 1, N_SUB), (event7, 4, 6, 1, N_SUB), (event8, 4, 8, 1, N_SUB)),
    )
    for c in range(n_steps):
        def gate_up(j):
            s = lax.rem(j, N_WB)

            @pl.when(j + N_WB - 1 < n_j)
            def _():
                for cp in wb_copies(j + N_WB - 1, lax.rem(j + N_WB - 1, N_WB)):
                    cp.start()

            for cp in wb_copies(j, s):
                cp.wait()
            both = jnp.dot(hb[c], wb[s], preferred_element_type=jnp.float32)
            gate = both[:, :HB]
            act[:, pl.ds(pl.multiple_of(j * HB, HB), HB)] = (jax.nn.silu(gate) * both[:, HB:]).astype(jnp.bfloat16)
            run(j, gate_tables[c])

        def down(j):
            s = lax.rem(j, N_DB)

            @pl.when(j + N_DB - 1 < n_d)
            def _():
                w2_copy(j + N_DB - 1, lax.rem(j + N_DB - 1, N_DB)).start()

            w2_copy(j, s).wait()
            part = jnp.dot(act[...], w2b[s], preferred_element_type=jnp.float32).astype(jnp.bfloat16)
            src[c, :, :, :, pl.ds(pl.multiple_of(j * DB, DB), DB)] = part.reshape(4, 2, piece, DB)

            @pl.when(lax.rem(j, per_cb) == per_cb - 1)
            def _():
                copy0(n_steps + c, j // per_cb).start()

            run(j, down_tables[c])
            if c == n_steps - 1:
                run(j, ((event1, n_steps + c, 2, 2, 4), (event2, n_steps + c, 5, 2, 3), (event3, n_steps + c, 8, 2, 1)))

        for s in range(N_DB - 1):
            w2_copy(s, s).start()
        loop(n_j, gate_up)
        if c < n_steps - 1:
            start_wb()
        loop(n_d, down)
        if c == 0:
            event8(1, 1)
            event4(2, 0)
            event4(2, 1)

    last = 2 * n_steps - 1
    for c in range(n_steps - 1):
        y_copy(c).start()
    event1(last, 4)
    event2(last, 3)
    event3(last, 1)
    event3(last, 2)
    event2(last, 4)
    event3(last, 3)
    event3(last, 4)
    finish_gather(last)
    y_copy(n_steps - 1).start()
    for c in range(n_steps):
        y_copy(c).wait()


def tail_layer(o, x_seq, w_o, w_gate, w_up, w_down, g_attn, g_mlp, axis):
    n_steps, n_seq, d_model = x_seq.shape
    piece = n_seq // 8
    n_hid = w_gate.shape[1]
    bf16 = jnp.bfloat16
    anym = pl.BlockSpec(memory_space=pl.ANY)
    dma = pltpu.SemaphoreType.DMA
    gains = jnp.stack([g_attn, g_mlp]).astype(jnp.float32)
    return pl.pallas_call(
        functools.partial(tail_kernel, axis),
        out_shape=jax.ShapeDtypeStruct((n_steps, n_seq, d_model), bf16),
        in_specs=[anym] * 7,
        out_specs=anym,
        scratch_shapes=[
            pltpu.VMEM(o.shape, jnp.float32),
            pltpu.VMEM((n_seq, w_o.shape[0]), bf16),
            pltpu.VMEM((n_steps, piece, d_model), bf16),
            pltpu.VMEM((n_steps, n_seq, d_model), bf16),
            pltpu.VMEM((n_steps, 4, 2, piece, d_model), bf16),
            pltpu.VMEM((n_steps, 4, piece, d_model), bf16),
            pltpu.VMEM((n_steps, 2, piece, d_model), bf16),
            pltpu.VMEM((n_steps, piece, d_model), bf16),
            pltpu.VMEM((n_seq, n_hid), bf16),
            pltpu.VMEM(w_o.shape, bf16),
            pltpu.VMEM((N_WB, d_model, 2 * HB), bf16),
            pltpu.VMEM((N_DB, n_hid, DB), bf16),
            pltpu.VMEM((2, d_model), jnp.float32),
            dma, dma, dma((N_CB,)), dma((N_WB, 2)), dma((N_DB,)), dma((n_steps,)), dma,
            dma((2 * n_steps, 4, N_CB)), dma((2 * n_steps, 4, N_CB)), dma((2 * n_steps, 7, N_SUB)), dma((2 * n_steps, 7, N_SUB)),
        ],
        compiler_params=pltpu.CompilerParams(collective_id=1, has_side_effects=True, vmem_limit_bytes=63 * MIB),
    )(o, x_seq, w_o, w_gate, w_up, w_down, gains)


def layer_steps(x_seq, cache_len, k_cache, v_cache, w_q, w_k, w_v, w_o, w_gate, w_up, w_down, g_q, g_k, g_attn, g_mlp, q_width, kv_width):
    n_steps, n_seq, _ = x_seq.shape
    hd = k_cache.shape[-1]
    q, kv = head_layer(x_seq, cache_len, w_q, w_k, w_v, g_q, g_k, q_width, kv_width, 'tp')
    o, k_out, v_out = attn_layer(cache_len, q, kv, k_cache, v_cache, w_q.shape[1] // hd, n_steps)
    y = tail_layer(o.reshape(n_seq * 16, hd), x_seq, w_o, w_gate, w_up, w_down, g_attn, g_mlp, 'tp')
    return y, k_out, v_out


def solution(mesh):
    tp_size = mesh.shape['tp']

    def local_run(x_seq, cache_len, k_cache, v_cache, w_q, w_k, w_v, w_o, w_gate, w_up, w_down, g_q, g_k, g_attn, g_mlp):
        return layer_steps(x_seq, cache_len, k_cache, v_cache, w_q, w_k, w_v, w_o, w_gate, w_up, w_down, g_q, g_k, g_attn, g_mlp, w_q.shape[1] * tp_size, w_k.shape[1] * tp_size)

    data_spec = P(None, 'dp', None)
    cache_spec = P('dp', 'tp', None, None)
    col_spec = P(None, 'tp')
    row_spec = P('tp', None)
    arg_specs = (data_spec, P('dp'), cache_spec, cache_spec, col_spec, col_spec, col_spec, row_spec, col_spec, col_spec, row_spec, P('tp'), P('tp'), P(None), P(None))
    out_specs = (data_spec, cache_spec, cache_spec)
    return jax.shard_map(local_run, mesh=mesh, in_specs=arg_specs, out_specs=out_specs, check_vma=False)
```

```python
import functools

import jax
import jax.numpy as jnp
from jax import lax
from jax.experimental import pallas as pl
from jax.experimental.pallas import tpu as pltpu
from jax.sharding import PartitionSpec as P

ROPE_THETA = 500000.0
NORM_EPS = 1e-6
MESH_ID = pl.DeviceIdType.MESH
MIB = 2**20


def rms_factor(sq_sum, full_width):
    return lax.rsqrt(sq_sum / full_width + NORM_EPS)


N_KB = 5


def head_kernel(axis, q_width, kv_width, x_hbm, wq_hbm, wk_hbm, wv_hbm, gq_hbm, gk_hbm, len_hbm, freq_hbm, q_ref, kv_ref,
                xv, wv, acc, raw, sums, parts, gq_ref, gk_ref, len_ref, freq_ref, in_sem, small_sem, s_sem, r_sem):
    n_steps, n_seq, d_model = x_hbm.shape
    wq_cols = wq_hbm.shape[1]
    hd = wk_hbm.shape[1]
    n_heads = wq_cols // hd
    kw = d_model // N_KB
    n_blk = n_steps * 2
    me = lax.axis_index(axis)

    def in_copies(kb):
        ks = pl.ds(pl.multiple_of(kb * kw, kw), kw)
        return (pltpu.make_async_copy(x_hbm.at[:, :, ks], xv.at[:, :, ks], in_sem.at[kb, 0]),
                pltpu.make_async_copy(wq_hbm.at[ks, :], wv.at[ks, 0:wq_cols], in_sem.at[kb, 1]),
                pltpu.make_async_copy(wk_hbm.at[ks, :], wv.at[ks, wq_cols:wq_cols + hd], in_sem.at[kb, 2]),
                pltpu.make_async_copy(wv_hbm.at[ks, :], wv.at[ks, wq_cols + hd:wq_cols + 2 * hd], in_sem.at[kb, 3]))

    for kb in range(N_KB):
        for cp in in_copies(kb):
            cp.start()

    small = [pltpu.make_async_copy(hbm, vmem, small_sem.at[n]) for n, (hbm, vmem) in enumerate(((gq_hbm, gq_ref), (gk_hbm, gk_ref), (len_hbm, len_ref), (freq_hbm, freq_ref)))]
    for cp in small:
        cp.start()

    bar = pltpu.get_barrier_semaphore()
    for i in range(1, 8):
        pl.semaphore_signal(bar, inc=1, device_id={axis: lax.rem(me + i, 8)}, device_id_type=MESH_ID)

    def project(kb, _):
        for cp in in_copies(kb):
            cp.wait()
        ks = pl.ds(pl.multiple_of(kb * kw, kw), kw)
        for t in range(n_steps):
            acc[t] += jnp.dot(xv[t, :, ks], wv[ks, :], preferred_element_type=jnp.float32)
        return 0

    acc[...] = jnp.zeros_like(acc)
    lax.fori_loop(0, N_KB, project, 0)

    lane = lax.broadcasted_iota(jnp.int32, (128, 128), 1)
    diag = lane == lax.broadcasted_iota(jnp.int32, (128, 128), 0)

    def to_row(col):
        return jnp.sum(jnp.where(diag, jnp.broadcast_to(col, (128, 128)), 0.0), axis=0, keepdims=True)

    def to_col(row):
        return jnp.sum(jnp.where(diag, jnp.broadcast_to(row, (128, 128)), 0.0), axis=1, keepdims=True)

    def rounded(v):
        return v.astype(jnp.bfloat16).astype(jnp.float32)

    sums[...] = jnp.zeros_like(sums)
    for blk in range(n_blk):
        t, half = blk // 2, blk % 2
        rows = slice(half * 128, half * 128 + 128)
        sq = None
        for g in range(n_heads):
            val = rounded(acc[t, rows, g * hd:(g + 1) * hd])
            raw[blk, g] = val
            sq = val * val if sq is None else sq + val * val
        sums[blk:blk + 1, :] = to_row(jnp.sum(sq, axis=-1, keepdims=True))
        val = rounded(acc[t, rows, wq_cols:wq_cols + hd])
        raw[blk, n_heads] = val
        sums[n_blk + blk:n_blk + blk + 1, :] = to_row(jnp.sum(val * val, axis=-1, keepdims=True))

    def exchange(i):
        return pltpu.make_async_remote_copy(src_ref=sums, dst_ref=parts.at[me], send_sem=s_sem.at[i - 1], recv_sem=r_sem.at[i - 1], device_id={axis: lax.rem(me + i, 8)}, device_id_type=MESH_ID)

    pl.semaphore_wait(bar, 7)
    for i in range(1, 8):
        exchange(i).start()
    parts[me] = sums[...]

    for blk in range(n_blk):
        t, half = blk // 2, blk % 2
        rows = slice(half * 128, half * 128 + 128)
        kv_ref[pl.ds(half * 1024 + 3 + t, 128, stride=8), :] = rounded(acc[t, rows, wq_cols + hd:wq_cols + 2 * hd])
    for half in range(2):
        zero = jnp.zeros((128, hd), jnp.float32)
        for slot in range(n_steps * n_heads, 16):
            q_ref[pl.ds(half * 2048 + slot, 128, stride=16), :] = zero
        for slot in range(2 * n_steps, 8):
            kv_ref[pl.ds(half * 1024 + slot, 128, stride=8), :] = zero
    for cp in small:
        cp.wait()
    low = lane < 64
    freq = freq_ref[...]
    lens = len_ref[...].astype(jnp.float32)
    angle = jnp.where(low, to_col(lens[0:1, :]), to_col(lens[1:2, :])) * freq
    cos_p = jnp.cos(angle)
    sin_p = jnp.sin(angle)
    cos_r = pltpu.roll(cos_p, 64, 1)
    sin_r = pltpu.roll(sin_p, 64, 1)
    cos_0 = (jnp.where(low, cos_p, cos_r), jnp.where(low, cos_r, cos_p))
    sin_0 = (jnp.where(low, sin_p, sin_r), jnp.where(low, sin_r, sin_p))

    for i in range(1, 8):
        exchange(i).wait()
    total = parts[0]
    for i in range(1, 8):
        total = total + parts[i]
    q_fac = rms_factor(total[0:n_blk], q_width)
    k_fac = rms_factor(total[n_blk:2 * n_blk], kv_width)
    gain_q = gq_ref[...].astype(jnp.float32).reshape(1, wq_cols)
    gain_k = gk_ref[...].astype(jnp.float32).reshape(1, hd)

    for blk in range(n_blk):
        t, half = blk // 2, blk % 2
        if t == 0:
            cos_t, sin_t = cos_0[half], sin_0[half]
        else:
            cos_s, sin_s = jnp.cos(freq * float(t)), jnp.sin(freq * float(t))
            cos_t = cos_0[half] * cos_s - sin_0[half] * sin_s
            sin_t = sin_0[half] * cos_s + cos_0[half] * sin_s
        sin_t = jnp.where(low, -sin_t, sin_t)

        def rope(val):
            return rounded(val * cos_t + pltpu.roll(val, 64, 1) * sin_t)

        fac = to_col(q_fac[blk:blk + 1, :])
        for g in range(n_heads):
            q_ref[pl.ds(half * 2048 + t * n_heads + g, 128, stride=16), :] = rope(raw[blk, g] * fac * gain_q[:, g * hd:(g + 1) * hd])
        fac = to_col(k_fac[blk:blk + 1, :])
        kv_ref[pl.ds(half * 1024 + t, 128, stride=8), :] = rope(raw[blk, n_heads] * fac * gain_k)


def head_layer(x_seq, cache_len, w_q, w_k, w_v, g_q, g_k, q_width, kv_width, axis):
    n_steps, n_seq, d_model = x_seq.shape
    hd = w_k.shape[1]
    cols = w_q.shape[1] + 2 * hd
    half_dim = hd // 2
    bf16, f32 = jnp.bfloat16, jnp.float32
    inv_freq = ROPE_THETA ** (-(jnp.arange(half_dim, dtype=f32) * (2.0 / hd)))
    freq = jnp.concatenate([inv_freq, inv_freq]).reshape(1, hd)
    anym = pl.BlockSpec(memory_space=pl.ANY)
    vmem = pl.BlockSpec(memory_space=pltpu.VMEM)
    dma = pltpu.SemaphoreType.DMA
    return pl.pallas_call(
        functools.partial(head_kernel, axis, q_width, kv_width),
        out_shape=(jax.ShapeDtypeStruct((n_seq * 16, hd), f32), jax.ShapeDtypeStruct((n_seq * 8, hd), f32)),
        in_specs=[anym] * 8,
        out_specs=(vmem, vmem),
        scratch_shapes=[
            pltpu.VMEM((n_steps, n_seq, d_model), bf16),
            pltpu.VMEM((d_model, cols), bf16),
            pltpu.VMEM((n_steps, n_seq, cols), f32),
            pltpu.VMEM((2 * n_steps, w_q.shape[1] // hd + 1, 128, hd), f32),
            pltpu.VMEM((16, 128), f32),
            pltpu.VMEM((8, 16, 128), f32),
            pltpu.VMEM(g_q.shape, bf16),
            pltpu.VMEM(g_k.shape, bf16),
            pltpu.VMEM((2, n_seq // 2), jnp.int32),
            pltpu.VMEM((1, hd), f32),
            dma((N_KB, 4)), dma((4,)), dma((7,)), dma((7,)),
        ],
        compiler_params=pltpu.CompilerParams(collective_id=0, has_side_effects=True, vmem_limit_bytes=63 * MIB),
    )(x_seq, w_q, w_k, w_v, g_q, g_k, cache_len.reshape(2, n_seq // 2), freq)


SEQ_GRP = 16
N_RING = 8
AHEAD = 4


def attn_kernel(n_heads, n_steps, len_ref, q_hbm, kv_hbm, k_hbm, v_hbm, o_hbm, ko_hbm, vo_hbm, qb, kvb, kb, vb, ob, in_sem, out_sem):
    n_seq, n_pos, hd = k_hbm.shape
    n_grp = n_seq // SEQ_GRP
    fixed = n_pos // 2
    scale = hd ** -0.5
    row = lax.broadcasted_iota(jnp.int32, (n_pos - fixed, hd), 0)
    s_step = lax.broadcasted_iota(jnp.int32, (16, n_pos - fixed), 0) // n_heads
    s_last = lax.broadcasted_iota(jnp.int32, (16, n_pos - fixed), 1) + fixed - s_step

    def copies(grp, pairs, sem):
        seqs = pl.ds(grp * SEQ_GRP, SEQ_GRP)
        s = lax.rem(grp, N_RING)
        return [pltpu.make_async_copy(hbm.at[seqs], vmem.at[s], sem.at[s, n]) if sem is in_sem else pltpu.make_async_copy(vmem.at[s], hbm.at[seqs], sem.at[s, n]) for n, (hbm, vmem) in enumerate(pairs)]

    def loads(grp):
        return copies(grp, ((k_hbm, kb), (v_hbm, vb), (q_hbm, qb), (kv_hbm, kvb)), in_sem)

    def stores(grp):
        return copies(grp, ((ko_hbm, kb), (vo_hbm, vb), (o_hbm, ob)), out_sem)

    for grp in range(AHEAD):
        for cp in loads(grp):
            cp.start()

    def group(grp, _):
        slot = lax.rem(grp, N_RING)

        @pl.when(grp + AHEAD < n_grp)
        def _():
            @pl.when(grp + AHEAD >= N_RING)
            def _():
                for cp in stores(grp + AHEAD - N_RING):
                    cp.wait()

            for cp in loads(grp + AHEAD):
                cp.start()

        for cp in loads(grp):
            cp.wait()
        idx = range(SEQ_GRP)
        lens = [len_ref[grp * SEQ_GRP + i] for i in idx]
        for i, length in zip(idx, lens):
            rel = row - (length - fixed)
            for buf, first in ((kb, 0), (vb, n_steps)):
                vals = buf[slot, i, fixed:n_pos, :].astype(jnp.float32)
                for t in range(n_steps):
                    vals = jnp.where(rel == t, kvb[slot, i, first + t:first + t + 1, :], vals)
                buf[slot, i, fixed:n_pos, :] = vals.astype(jnp.bfloat16)
        scores = [lax.dot_general(qb[slot, i].astype(jnp.bfloat16), kb[slot, i], (((1,), (1,)), ((), ())), preferred_element_type=jnp.float32) for i in idx]
        probs = []
        sums = []
        for s, length in zip(scores, lens):
            lo = s[:, 0:fixed] * scale
            hi = jnp.where(s_last <= length, s[:, fixed:n_pos] * scale, -jnp.inf)
            top = jnp.max(jnp.maximum(lo, hi), axis=-1, keepdims=True)
            lo = jnp.exp(lo - top)
            hi = jnp.exp(hi - top)
            sums.append(jnp.sum(lo + hi, axis=-1, keepdims=True))
            probs.append(jnp.concatenate([lo.astype(jnp.bfloat16), hi.astype(jnp.bfloat16)], axis=-1))
        for i, p, total in zip(idx, probs, sums):
            ob[slot, i] = jnp.dot(p, vb[slot, i], preferred_element_type=jnp.float32) / total
        for cp in stores(grp):
            cp.start()
        return 0

    lax.fori_loop(0, n_grp, group, 0)

    def drain(grp, _):
        for cp in stores(grp):
            cp.wait()
        return 0

    lax.fori_loop(n_grp - N_RING, n_grp, drain, 0)


def attn_layer(cache_len, q, kv, k_cache, v_cache, n_heads, n_steps):
    n_seq, _, n_pos, hd = k_cache.shape
    bf16, f32 = jnp.bfloat16, jnp.float32
    anym = pl.BlockSpec(memory_space=pl.ANY)
    dma = pltpu.SemaphoreType.DMA
    ring = (N_RING, SEQ_GRP)
    o, k_out, v_out = pl.pallas_call(
        functools.partial(attn_kernel, n_heads, n_steps),
        out_shape=(jax.ShapeDtypeStruct((n_seq, 16, hd), f32), jax.ShapeDtypeStruct((n_seq, n_pos, hd), bf16), jax.ShapeDtypeStruct((n_seq, n_pos, hd), bf16)),
        in_specs=[pl.BlockSpec(memory_space=pltpu.SMEM)] + [anym] * 4,
        out_specs=(anym, anym, anym),
        scratch_shapes=[
            pltpu.VMEM(ring + (16, hd), f32),
            pltpu.VMEM(ring + (8, hd), f32),
            pltpu.VMEM(ring + (n_pos, hd), bf16),
            pltpu.VMEM(ring + (n_pos, hd), bf16),
            pltpu.VMEM(ring + (16, hd), f32),
            dma((N_RING, 4)), dma((N_RING, 3)),
        ],
        compiler_params=pltpu.CompilerParams(vmem_limit_bytes=63 * MIB),
    )(cache_len, q.reshape(n_seq, 16, hd), kv.reshape(n_seq, 8, hd), k_cache.reshape(n_seq, n_pos, hd), v_cache.reshape(n_seq, n_pos, hd))
    return o, k_out.reshape(k_cache.shape), v_out.reshape(v_cache.shape)


N_CB = 5
N_SUB = 2
N_WB = 4
N_DB = 3
HB = 128
DB = 512


def tail_kernel(axis, o_hbm, x_hbm, wo_hbm, w1_hbm, w3_hbm, w2_hbm, ga_hbm, gm_hbm, y_hbm,
                on, ob, xp, hb, src, recv0, recv1, recv2, act, wob, wb, w2b, ga_ref, gm_ref,
                o_sem, x_sem, wo_sem, wb_sem, w2_sem, y_sem, gain_sem, s_sem, r_sem, g_ssem, g_rsem):
    n_steps, n_seq, d_model = x_hbm.shape
    piece = n_seq // 8
    sub_rows = piece // N_SUB
    cw = d_model // N_CB
    n_hid = w1_hbm.shape[1]
    n_j = n_hid // HB
    n_d = d_model // DB
    per_cb = n_d // N_CB
    hd = o_hbm.shape[1]
    n_heads = wo_hbm.shape[0] // hd

    me = lax.axis_index(axis)
    core = lax.rem(me, 2)
    xb = lax.rem(me // 2, 2)
    yb = me // 4
    first_bit = core * yb + (1 - core) * xb
    second_bit = core * xb + (1 - core) * yb
    fw = 1 + core
    sw = 2 - core
    partner = me + 1 - 2 * core
    fpeer = me + (1 - 2 * first_bit) * 2 * fw
    speer = me + (1 - 2 * second_bit) * 2 * sw
    fspeer = fpeer + speer - me

    def remote(src_ref, dst_ref, send, recv, dev):
        return pltpu.make_async_remote_copy(src_ref=src_ref, dst_ref=dst_ref, send_sem=send, recv_sem=recv, device_id={axis: dev}, device_id_type=MESH_ID)

    o_copy = pltpu.make_async_copy(o_hbm, on, o_sem)
    o_copy.start()

    def wo_copy(cb):
        return pltpu.make_async_copy(wo_hbm.at[:, pl.ds(cb * cw, cw)], wob.at[:, pl.ds(cb * cw, cw)], wo_sem.at[cb])

    for cb in range(N_CB):
        wo_copy(cb).start()
    gain_copies = (pltpu.make_async_copy(ga_hbm, ga_ref, gain_sem.at[0]), pltpu.make_async_copy(gm_hbm, gm_ref, gain_sem.at[1]))
    for cp in gain_copies:
        cp.start()
    x_copy = pltpu.make_async_copy(x_hbm.at[:, pl.ds(pl.multiple_of(piece * me, piece), piece), :], xp, x_sem)
    x_copy.start()

    def wb_copies(j, s):
        col = pl.ds(pl.multiple_of(j * HB, HB), HB)
        return (pltpu.make_async_copy(w1_hbm.at[:, col], wb.at[s, :, 0:HB], wb_sem.at[s, 0]),
                pltpu.make_async_copy(w3_hbm.at[:, col], wb.at[s, :, HB:2 * HB], wb_sem.at[s, 1]))

    def w2_copy(j, s):
        return pltpu.make_async_copy(w2_hbm.at[:, pl.ds(pl.multiple_of(j * DB, DB), DB)], w2b.at[s], w2_sem.at[s])

    def start_wb():
        for s in range(N_WB - 1):
            for cp in wb_copies(s, s):
                cp.start()

    start_wb()

    bar = pltpu.get_barrier_semaphore()
    for dev in (partner, fpeer, speer):
        pl.semaphore_signal(bar, inc=1, device_id={axis: dev}, device_id_type=MESH_ID)
    pl.semaphore_wait(bar, 3)

    def cols_of(cb):
        return pl.ds(pl.multiple_of(cb * cw, cw), cw)

    def copy0(inst, cb):
        c = inst % n_steps
        return remote(src.at[c, :, 1 - core, :, cols_of(cb)], recv0.at[c, :, :, cols_of(cb)], s_sem.at[inst, 0, cb], r_sem.at[inst, 0, cb], partner)

    def copy1(inst, cb, k):
        c = inst % n_steps
        sb = (1 - second_bit) if k == 0 else second_bit
        idx = (1 - first_bit) * fw + sb * sw
        return remote(recv0.at[c, idx, :, cols_of(cb)], recv1.at[c, k, :, cols_of(cb)], s_sem.at[inst, 1 + k, cb], r_sem.at[inst, 1 + k, cb], fpeer)

    def copy2(inst, cb):
        c = inst % n_steps
        return remote(recv1.at[c, 0, :, cols_of(cb)], recv2.at[c, :, cols_of(cb)], s_sem.at[inst, 3, cb], r_sem.at[inst, 3, cb], speer)

    def f32(v):
        return v.astype(jnp.float32)

    def event1(inst, cb):
        c = inst % n_steps
        copy0(inst, cb).wait_recv()
        cols = cols_of(cb)

        def add(i, _):
            recv0[c, i, :, cols] = (f32(src[c, i, core, :, cols]) + f32(recv0[c, i, :, cols])).astype(jnp.bfloat16)
            return 0

        lax.fori_loop(0, 4, add, 0)
        copy1(inst, cb, 0).start()
        copy1(inst, cb, 1).start()

    def event2(inst, cb):
        c = inst % n_steps
        copy1(inst, cb, 0).wait_recv()
        cols = cols_of(cb)
        idx = first_bit * fw + (1 - second_bit) * sw
        recv1[c, 0, :, cols] = (f32(recv0[c, idx, :, cols]) + f32(recv1[c, 0, :, cols])).astype(jnp.bfloat16)
        copy2(inst, cb).start()

    def event3(inst, cb):
        c = inst % n_steps
        copy1(inst, cb, 1).wait_recv()
        copy2(inst, cb).wait_recv()
        cols = cols_of(cb)
        idx = first_bit * fw + second_bit * sw
        recv2[c, :, cols] = (f32(recv0[c, idx, :, cols]) + f32(recv1[c, 1, :, cols]) + f32(recv2[c, :, cols])).astype(jnp.bfloat16)

    def gcopy(inst, k, sub):
        c = inst % n_steps
        who, dev = ((me, speer), (me, fpeer), (me, partner), (speer, fpeer), (speer, partner), (fpeer, partner), (fspeer, partner))[k]
        part = hb.at[c, pl.ds(pl.multiple_of(who * piece + sub * sub_rows, sub_rows), sub_rows), :]
        return remote(part, part, g_ssem.at[inst, k, sub], g_rsem.at[inst, k, sub], dev)

    def event4(inst, sub):
        c = inst % n_steps
        attn = inst < n_steps

        @pl.when(sub == 0)
        def _():
            def drain(cb, _):
                copy0(inst, cb).wait_send()
                copy1(inst, cb, 0).wait_send()
                copy1(inst, cb, 1).wait_send()
                copy2(inst, cb).wait_send()
                return 0

            lax.fori_loop(0, N_CB, drain, 0)

        r = pl.ds(pl.multiple_of(sub * sub_rows, sub_rows), sub_rows)
        hr = pl.ds(pl.multiple_of(me * piece + sub * sub_rows, sub_rows), sub_rows)
        a = f32(recv2[c, r, :])
        factor = rms_factor(jnp.sum(a * a, axis=-1, keepdims=True), d_model)
        base = f32(xp[c, r, :]) if attn else f32(hb[c, hr, :])
        gain = f32((ga_ref if attn else gm_ref)[...]).reshape(1, d_model)
        hb[c, hr, :] = (base + a * factor * gain).astype(jnp.bfloat16)
        for k in (1, 0, 2):
            gcopy(inst, k, sub).start()

    def event5(inst, sub):
        gcopy(inst, 0, sub).wait_recv()
        gcopy(inst, 3, sub).start()
        gcopy(inst, 4, sub).start()
        gcopy(inst, 1, sub).wait_recv()
        gcopy(inst, 5, sub).start()

    def event7(inst, sub):
        gcopy(inst, 3, sub).wait_recv()
        gcopy(inst, 6, sub).start()

    def event8(inst, sub):
        for k in (2, 4, 5, 6):
            gcopy(inst, k, sub).wait_recv()
        for k in range(7):
            gcopy(inst, k, sub).wait_send()

    def run(j, table):
        for event, inst, start, every, count in table:
            k = j - start
            cond = (k >= 0) & (k < every * count)
            if every > 1:
                cond = cond & (lax.rem(k, every) == 0)

            @pl.when(cond)
            def _():
                event(inst, k // every)

    def loop(n, fn):
        lax.fori_loop(0, n, lambda i, _: (fn(i), 0)[1], 0)

    def out_proj(c):
        for g in range(n_heads):
            ob[:, g * hd:(g + 1) * hd] = on[pl.ds(c * n_heads + g, n_seq, stride=16), :].astype(jnp.bfloat16)

        def step(cb):
            part = jnp.dot(ob[...], wob[:, cols_of(cb)], preferred_element_type=jnp.float32).astype(jnp.bfloat16)
            src[c, :, :, :, cols_of(cb)] = part.reshape(4, 2, piece, cw)
            copy0(c, cb).start()

        loop(N_CB, step)

    def y_copy(c):
        return pltpu.make_async_copy(hb.at[c], y_hbm.at[c], y_sem.at[c])

    o_copy.wait()
    for cb in range(N_CB):
        wo_copy(cb).wait()
    out_proj(0)
    loop(N_CB, functools.partial(event1, 0))
    out_proj(1)
    out_proj(2)
    x_copy.wait()
    for cp in gain_copies:
        cp.wait()

    def finish_reduce(inst):
        def step(k):
            @pl.when(k < N_CB)
            def _():
                event2(inst, k)

            @pl.when(k > 0)
            def _():
                event3(inst, k - 1)

        loop(N_CB + 1, step)

    def finish_gather(inst):
        loop(N_SUB, functools.partial(event4, inst))
        loop(N_SUB, functools.partial(event5, inst))
        loop(N_SUB, functools.partial(event7, inst))
        loop(N_SUB, functools.partial(event8, inst))

    finish_reduce(0)
    finish_gather(0)

    gate_tables = (
        ((event1, 1, 0, 1, N_CB), (event2, 1, 4, 2, N_CB), (event3, 1, 9, 2, N_CB), (event4, 1, 18, 1, N_SUB), (event1, 2, 20, 1, N_CB)),
        ((event1, 3, 0, 1, N_CB), (event2, 3, 6, 3, N_CB), (event5, 2, 10, 1, N_SUB), (event3, 3, 10, 3, N_CB), (event7, 2, 17, 1, N_SUB), (event8, 2, 20, 1, N_SUB), (event4, 3, 24, 1, N_SUB)),
        ((event1, 4, 0, 1, N_CB), (event7, 3, 2, 1, N_SUB), (event2, 4, 6, 2, N_CB), (event8, 3, 7, 1, N_SUB), (event3, 4, 10, 2, N_CB), (event4, 4, 19, 1, N_SUB)),
    )
    down_tables = (
        ((event2, 2, 0, 1, N_CB), (event3, 2, 4, 1, N_CB), (event5, 1, 3, 1, N_SUB), (event7, 1, 7, 1, N_SUB), (event8, 1, 9, 1, 1)),
        ((event5, 3, 6, 1, N_SUB),),
        ((event5, 4, 3, 1, N_SUB), (event7, 4, 6, 1, N_SUB), (event8, 4, 8, 1, N_SUB)),
    )
    for c in range(n_steps):
        def gate_up(j):
            s = lax.rem(j, N_WB)

            @pl.when(j + N_WB - 1 < n_j)
            def _():
                for cp in wb_copies(j + N_WB - 1, lax.rem(j + N_WB - 1, N_WB)):
                    cp.start()

            for cp in wb_copies(j, s):
                cp.wait()
            both = jnp.dot(hb[c], wb[s], preferred_element_type=jnp.float32)
            gate = both[:, :HB]
            act[:, pl.ds(pl.multiple_of(j * HB, HB), HB)] = (jax.nn.silu(gate) * both[:, HB:]).astype(jnp.bfloat16)
            run(j, gate_tables[c])

        def down(j):
            s = lax.rem(j, N_DB)

            @pl.when(j + N_DB - 1 < n_d)
            def _():
                w2_copy(j + N_DB - 1, lax.rem(j + N_DB - 1, N_DB)).start()

            w2_copy(j, s).wait()
            part = jnp.dot(act[...], w2b[s], preferred_element_type=jnp.float32).astype(jnp.bfloat16)
            src[c, :, :, :, pl.ds(pl.multiple_of(j * DB, DB), DB)] = part.reshape(4, 2, piece, DB)

            @pl.when(lax.rem(j, per_cb) == per_cb - 1)
            def _():
                copy0(n_steps + c, j // per_cb).start()

            run(j, down_tables[c])
            if c == n_steps - 1:
                run(j, ((event1, n_steps + c, 2, 2, 4), (event2, n_steps + c, 5, 2, 3), (event3, n_steps + c, 8, 2, 1)))

        for s in range(N_DB - 1):
            w2_copy(s, s).start()
        loop(n_j, gate_up)
        if c < n_steps - 1:
            start_wb()
        loop(n_d, down)
        if c == 0:
            event8(1, 1)
            event4(2, 0)
            event4(2, 1)

    last = 2 * n_steps - 1
    for c in range(n_steps - 1):
        y_copy(c).start()
    event1(last, 4)
    event2(last, 3)
    event3(last, 1)
    event3(last, 2)
    event2(last, 4)
    event3(last, 3)
    event3(last, 4)
    finish_gather(last)
    y_copy(n_steps - 1).start()
    for c in range(n_steps):
        y_copy(c).wait()


def tail_layer(o, x_seq, w_o, w_gate, w_up, w_down, g_attn, g_mlp, axis):
    n_steps, n_seq, d_model = x_seq.shape
    piece = n_seq // 8
    n_hid = w_gate.shape[1]
    bf16 = jnp.bfloat16
    anym = pl.BlockSpec(memory_space=pl.ANY)
    dma = pltpu.SemaphoreType.DMA
    return pl.pallas_call(
        functools.partial(tail_kernel, axis),
        out_shape=jax.ShapeDtypeStruct((n_steps, n_seq, d_model), bf16),
        in_specs=[anym] * 8,
        out_specs=anym,
        scratch_shapes=[
            pltpu.VMEM(o.shape, jnp.float32),
            pltpu.VMEM((n_seq, w_o.shape[0]), bf16),
            pltpu.VMEM((n_steps, piece, d_model), bf16),
            pltpu.VMEM((n_steps, n_seq, d_model), bf16),
            pltpu.VMEM((n_steps, 4, 2, piece, d_model), bf16),
            pltpu.VMEM((n_steps, 4, piece, d_model), bf16),
            pltpu.VMEM((n_steps, 2, piece, d_model), bf16),
            pltpu.VMEM((n_steps, piece, d_model), bf16),
            pltpu.VMEM((n_seq, n_hid), bf16),
            pltpu.VMEM(w_o.shape, bf16),
            pltpu.VMEM((N_WB, d_model, 2 * HB), bf16),
            pltpu.VMEM((N_DB, n_hid, DB), bf16),
            pltpu.VMEM((d_model,), bf16),
            pltpu.VMEM((d_model,), bf16),
            dma, dma, dma((N_CB,)), dma((N_WB, 2)), dma((N_DB,)), dma((n_steps,)), dma((2,)),
            dma((2 * n_steps, 4, N_CB)), dma((2 * n_steps, 4, N_CB)), dma((2 * n_steps, 7, N_SUB)), dma((2 * n_steps, 7, N_SUB)),
        ],
        compiler_params=pltpu.CompilerParams(collective_id=1, has_side_effects=True, vmem_limit_bytes=63 * MIB),
    )(o, x_seq, w_o, w_gate, w_up, w_down, g_attn, g_mlp)


def layer_steps(x_seq, cache_len, k_cache, v_cache, w_q, w_k, w_v, w_o, w_gate, w_up, w_down, g_q, g_k, g_attn, g_mlp, q_width, kv_width):
    n_steps, n_seq, _ = x_seq.shape
    hd = k_cache.shape[-1]
    q, kv = head_layer(x_seq, cache_len, w_q, w_k, w_v, g_q, g_k, q_width, kv_width, 'tp')
    o, k_out, v_out = attn_layer(cache_len, q, kv, k_cache, v_cache, w_q.shape[1] // hd, n_steps)
    y = tail_layer(o.reshape(n_seq * 16, hd), x_seq, w_o, w_gate, w_up, w_down, g_attn, g_mlp, 'tp')
    return y, k_out, v_out


def solution(mesh):
    tp_size = mesh.shape['tp']

    def local_run(x_seq, cache_len, k_cache, v_cache, w_q, w_k, w_v, w_o, w_gate, w_up, w_down, g_q, g_k, g_attn, g_mlp):
        return layer_steps(x_seq, cache_len, k_cache, v_cache, w_q, w_k, w_v, w_o, w_gate, w_up, w_down, g_q, g_k, g_attn, g_mlp, w_q.shape[1] * tp_size, w_k.shape[1] * tp_size)

    data_spec = P(None, 'dp', None)
    cache_spec = P('dp', 'tp', None, None)
    col_spec = P(None, 'tp')
    row_spec = P('tp', None)
    arg_specs = (data_spec, P('dp'), cache_spec, cache_spec, col_spec, col_spec, col_spec, row_spec, col_spec, col_spec, row_spec, P('tp'), P('tp'), P(None), P(None))
    out_specs = (data_spec, cache_spec, cache_spec)
    return jax.shard_map(local_run, mesh=mesh, in_specs=arg_specs, out_specs=out_specs, check_vma=False)
```

```python
import functools

import jax
import jax.numpy as jnp
from jax import lax
from jax.experimental import pallas as pl
from jax.experimental.pallas import tpu as pltpu
from jax.sharding import PartitionSpec as P

ROPE_THETA = 500000.0
NORM_EPS = 1e-6
MESH_ID = pl.DeviceIdType.MESH
MIB = 2**20


def rms_factor(sq_sum, full_width):
    return lax.rsqrt(sq_sum / full_width + NORM_EPS)


N_KB = 5


def head_kernel(axis, q_width, kv_width, x_hbm, wq_hbm, wk_hbm, wv_hbm, gq_hbm, gk_hbm, len_hbm, freq_hbm, q_ref, kv_ref,
                xv, wv, acc, raw, sums, parts, gq_ref, gk_ref, len_ref, freq_ref, in_sem, small_sem, s_sem, r_sem):
    n_steps, n_seq, d_model = x_hbm.shape
    wq_cols = wq_hbm.shape[1]
    hd = wk_hbm.shape[1]
    n_heads = wq_cols // hd
    kw = d_model // N_KB
    n_blk = n_steps * 2
    me = lax.axis_index(axis)

    def in_copies(kb):
        ks = pl.ds(pl.multiple_of(kb * kw, kw), kw)
        return (pltpu.make_async_copy(x_hbm.at[:, :, ks], xv.at[:, :, ks], in_sem.at[kb, 0]),
                pltpu.make_async_copy(wq_hbm.at[ks, :], wv.at[ks, 0:wq_cols], in_sem.at[kb, 1]),
                pltpu.make_async_copy(wk_hbm.at[ks, :], wv.at[ks, wq_cols:wq_cols + hd], in_sem.at[kb, 2]),
                pltpu.make_async_copy(wv_hbm.at[ks, :], wv.at[ks, wq_cols + hd:wq_cols + 2 * hd], in_sem.at[kb, 3]))

    for kb in range(N_KB):
        for cp in in_copies(kb):
            cp.start()

    small = [pltpu.make_async_copy(hbm, vmem, small_sem.at[n]) for n, (hbm, vmem) in enumerate(((gq_hbm, gq_ref), (gk_hbm, gk_ref), (len_hbm, len_ref), (freq_hbm, freq_ref)))]
    for cp in small:
        cp.start()

    bar = pltpu.get_barrier_semaphore()
    for i in range(1, 8):
        pl.semaphore_signal(bar, inc=1, device_id={axis: lax.rem(me + i, 8)}, device_id_type=MESH_ID)

    def project(kb, _):
        for cp in in_copies(kb):
            cp.wait()
        ks = pl.ds(pl.multiple_of(kb * kw, kw), kw)
        for t in range(n_steps):
            acc[t] += jnp.dot(xv[t, :, ks], wv[ks, :], preferred_element_type=jnp.float32)
        return 0

    acc[...] = jnp.zeros_like(acc)
    lax.fori_loop(0, N_KB, project, 0)

    lane = lax.broadcasted_iota(jnp.int32, (128, 128), 1)
    diag = lane == lax.broadcasted_iota(jnp.int32, (128, 128), 0)

    def to_row(col):
        return jnp.sum(jnp.where(diag, jnp.broadcast_to(col, (128, 128)), 0.0), axis=0, keepdims=True)

    def to_col(row):
        return jnp.sum(jnp.where(diag, jnp.broadcast_to(row, (128, 128)), 0.0), axis=1, keepdims=True)

    def rounded(v):
        return v.astype(jnp.bfloat16).astype(jnp.float32)

    sums[...] = jnp.zeros_like(sums)
    for blk in range(n_blk):
        t, half = blk // 2, blk % 2
        rows = slice(half * 128, half * 128 + 128)
        sq = None
        for g in range(n_heads):
            val = rounded(acc[t, rows, g * hd:(g + 1) * hd])
            raw[blk, g] = val
            sq = val * val if sq is None else sq + val * val
        sums[blk:blk + 1, :] = to_row(jnp.sum(sq, axis=-1, keepdims=True))
        val = rounded(acc[t, rows, wq_cols:wq_cols + hd])
        raw[blk, n_heads] = val
        sums[n_blk + blk:n_blk + blk + 1, :] = to_row(jnp.sum(val * val, axis=-1, keepdims=True))

    def exchange(i):
        return pltpu.make_async_remote_copy(src_ref=sums, dst_ref=parts.at[me], send_sem=s_sem.at[i - 1], recv_sem=r_sem.at[i - 1], device_id={axis: lax.rem(me + i, 8)}, device_id_type=MESH_ID)

    pl.semaphore_wait(bar, 7)
    for i in range(1, 8):
        exchange(i).start()
    parts[me] = sums[...]

    for blk in range(n_blk):
        t, half = blk // 2, blk % 2
        rows = slice(half * 128, half * 128 + 128)
        kv_ref[pl.ds(half * 1024 + 3 + t, 128, stride=8), :] = rounded(acc[t, rows, wq_cols + hd:wq_cols + 2 * hd])
    for half in range(2):
        zero = jnp.zeros((128, hd), jnp.float32)
        for slot in range(n_steps * n_heads, 16):
            q_ref[pl.ds(half * 2048 + slot, 128, stride=16), :] = zero
        for slot in range(2 * n_steps, 8):
            kv_ref[pl.ds(half * 1024 + slot, 128, stride=8), :] = zero
    for cp in small:
        cp.wait()
    low = lane < 64
    freq = freq_ref[...]
    lens = len_ref[...].astype(jnp.float32)
    angle = jnp.where(low, to_col(lens[0:1, :]), to_col(lens[1:2, :])) * freq
    cos_p = jnp.cos(angle)
    sin_p = jnp.sin(angle)
    cos_r = pltpu.roll(cos_p, 64, 1)
    sin_r = pltpu.roll(sin_p, 64, 1)
    cos_0 = (jnp.where(low, cos_p, cos_r), jnp.where(low, cos_r, cos_p))
    sin_0 = (jnp.where(low, sin_p, sin_r), jnp.where(low, sin_r, sin_p))

    for i in range(1, 8):
        exchange(i).wait()
    total = parts[0]
    for i in range(1, 8):
        total = total + parts[i]
    q_fac = rms_factor(total[0:n_blk], q_width)
    k_fac = rms_factor(total[n_blk:2 * n_blk], kv_width)
    gain_q = gq_ref[...].astype(jnp.float32).reshape(1, wq_cols)
    gain_k = gk_ref[...].astype(jnp.float32).reshape(1, hd)

    for blk in range(n_blk):
        t, half = blk // 2, blk % 2
        if t == 0:
            cos_t, sin_t = cos_0[half], sin_0[half]
        else:
            cos_s, sin_s = jnp.cos(freq * float(t)), jnp.sin(freq * float(t))
            cos_t = cos_0[half] * cos_s - sin_0[half] * sin_s
            sin_t = sin_0[half] * cos_s + cos_0[half] * sin_s
        sin_t = jnp.where(low, -sin_t, sin_t)

        def rope(val):
            return rounded(val * cos_t + pltpu.roll(val, 64, 1) * sin_t)

        fac = to_col(q_fac[blk:blk + 1, :])
        for g in range(n_heads):
            q_ref[pl.ds(half * 2048 + t * n_heads + g, 128, stride=16), :] = rope(raw[blk, g] * fac * gain_q[:, g * hd:(g + 1) * hd])
        fac = to_col(k_fac[blk:blk + 1, :])
        kv_ref[pl.ds(half * 1024 + t, 128, stride=8), :] = rope(raw[blk, n_heads] * fac * gain_k)


def head_layer(x_seq, cache_len, w_q, w_k, w_v, g_q, g_k, q_width, kv_width, axis):
    n_steps, n_seq, d_model = x_seq.shape
    hd = w_k.shape[1]
    cols = w_q.shape[1] + 2 * hd
    half_dim = hd // 2
    bf16, f32 = jnp.bfloat16, jnp.float32
    inv_freq = ROPE_THETA ** (-(jnp.arange(half_dim, dtype=f32) * (2.0 / hd)))
    freq = jnp.concatenate([inv_freq, inv_freq]).reshape(1, hd)
    anym = pl.BlockSpec(memory_space=pl.ANY)
    vmem = pl.BlockSpec(memory_space=pltpu.VMEM)
    dma = pltpu.SemaphoreType.DMA
    return pl.pallas_call(
        functools.partial(head_kernel, axis, q_width, kv_width),
        out_shape=(jax.ShapeDtypeStruct((n_seq * 16, hd), f32), jax.ShapeDtypeStruct((n_seq * 8, hd), f32)),
        in_specs=[anym] * 8,
        out_specs=(vmem, vmem),
        scratch_shapes=[
            pltpu.VMEM((n_steps, n_seq, d_model), bf16),
            pltpu.VMEM((d_model, cols), bf16),
            pltpu.VMEM((n_steps, n_seq, cols), f32),
            pltpu.VMEM((2 * n_steps, w_q.shape[1] // hd + 1, 128, hd), f32),
            pltpu.VMEM((16, 128), f32),
            pltpu.VMEM((8, 16, 128), f32),
            pltpu.VMEM(g_q.shape, bf16),
            pltpu.VMEM(g_k.shape, bf16),
            pltpu.VMEM((2, n_seq // 2), jnp.int32),
            pltpu.VMEM((1, hd), f32),
            dma((N_KB, 4)), dma((4,)), dma((7,)), dma((7,)),
        ],
        compiler_params=pltpu.CompilerParams(collective_id=0, has_side_effects=True, vmem_limit_bytes=63 * MIB),
    )(x_seq, w_q, w_k, w_v, g_q, g_k, cache_len.reshape(2, n_seq // 2), freq)


SEQ_GRP = 16
N_RING = 8
AHEAD = 4


def attn_kernel(n_heads, n_steps, len_ref, q_hbm, kv_hbm, k_hbm, v_hbm, o_hbm, ko_hbm, vo_hbm, qb, kvb, kb, vb, ob, in_sem, out_sem):
    n_seq, n_pos, hd = k_hbm.shape
    n_grp = n_seq // SEQ_GRP
    fixed = n_pos // 2
    scale = hd ** -0.5
    row = lax.broadcasted_iota(jnp.int32, (n_pos - fixed, hd), 0)
    s_step = lax.broadcasted_iota(jnp.int32, (16, n_pos - fixed), 0) // n_heads
    s_last = lax.broadcasted_iota(jnp.int32, (16, n_pos - fixed), 1) + fixed - s_step

    def copies(grp, pairs, sem):
        seqs = pl.ds(grp * SEQ_GRP, SEQ_GRP)
        s = lax.rem(grp, N_RING)
        return [pltpu.make_async_copy(hbm.at[seqs], vmem.at[s], sem.at[s, n]) if sem is in_sem else pltpu.make_async_copy(vmem.at[s], hbm.at[seqs], sem.at[s, n]) for n, (hbm, vmem) in enumerate(pairs)]

    def loads(grp):
        return copies(grp, ((k_hbm, kb), (v_hbm, vb), (q_hbm, qb), (kv_hbm, kvb)), in_sem)

    def stores(grp):
        return copies(grp, ((ko_hbm, kb), (vo_hbm, vb), (o_hbm, ob)), out_sem)

    for grp in range(AHEAD):
        for cp in loads(grp):
            cp.start()

    def group(grp, _):
        slot = lax.rem(grp, N_RING)

        @pl.when(grp + AHEAD < n_grp)
        def _():
            @pl.when(grp + AHEAD >= N_RING)
            def _():
                for cp in stores(grp + AHEAD - N_RING):
                    cp.wait()

            for cp in loads(grp + AHEAD):
                cp.start()

        for cp in loads(grp):
            cp.wait()
        idx = range(SEQ_GRP)
        lens = [len_ref[grp * SEQ_GRP + i] for i in idx]
        for i, length in zip(idx, lens):
            rel = row - (length - fixed)
            for buf, first in ((kb, 0), (vb, n_steps)):
                vals = buf[slot, i, fixed:n_pos, :].astype(jnp.float32)
                for t in range(n_steps):
                    vals = jnp.where(rel == t, kvb[slot, i, first + t:first + t + 1, :], vals)
                buf[slot, i, fixed:n_pos, :] = vals.astype(jnp.bfloat16)
        scores = [lax.dot_general(qb[slot, i].astype(jnp.bfloat16), kb[slot, i], (((1,), (1,)), ((), ())), preferred_element_type=jnp.float32) for i in idx]
        probs = []
        sums = []
        for s, length in zip(scores, lens):
            lo = s[:, 0:fixed] * scale
            hi = jnp.where(s_last <= length, s[:, fixed:n_pos] * scale, -jnp.inf)
            top = jnp.max(jnp.maximum(lo, hi), axis=-1, keepdims=True)
            lo = jnp.exp(lo - top)
            hi = jnp.exp(hi - top)
            sums.append(jnp.sum(lo + hi, axis=-1, keepdims=True))
            probs.append(jnp.concatenate([lo.astype(jnp.bfloat16), hi.astype(jnp.bfloat16)], axis=-1))
        for i, p, total in zip(idx, probs, sums):
            ob[slot, i] = jnp.dot(p, vb[slot, i], preferred_element_type=jnp.float32) / total
        for cp in stores(grp):
            cp.start()
        return 0

    lax.fori_loop(0, n_grp, group, 0)

    def drain(grp, _):
        for cp in stores(grp):
            cp.wait()
        return 0

    lax.fori_loop(n_grp - N_RING, n_grp, drain, 0)


def attn_layer(cache_len, q, kv, k_cache, v_cache, n_heads, n_steps):
    n_seq, _, n_pos, hd = k_cache.shape
    bf16, f32 = jnp.bfloat16, jnp.float32
    anym = pl.BlockSpec(memory_space=pl.ANY)
    dma = pltpu.SemaphoreType.DMA
    ring = (N_RING, SEQ_GRP)
    o, k_out, v_out = pl.pallas_call(
        functools.partial(attn_kernel, n_heads, n_steps),
        out_shape=(jax.ShapeDtypeStruct((n_seq, 16, hd), f32), jax.ShapeDtypeStruct((n_seq, n_pos, hd), bf16), jax.ShapeDtypeStruct((n_seq, n_pos, hd), bf16)),
        in_specs=[pl.BlockSpec(memory_space=pltpu.SMEM)] + [anym] * 4,
        out_specs=(anym, anym, anym),
        scratch_shapes=[
            pltpu.VMEM(ring + (16, hd), f32),
            pltpu.VMEM(ring + (8, hd), f32),
            pltpu.VMEM(ring + (n_pos, hd), bf16),
            pltpu.VMEM(ring + (n_pos, hd), bf16),
            pltpu.VMEM(ring + (16, hd), f32),
            dma((N_RING, 4)), dma((N_RING, 3)),
        ],
        compiler_params=pltpu.CompilerParams(vmem_limit_bytes=63 * MIB),
    )(cache_len, q.reshape(n_seq, 16, hd), kv.reshape(n_seq, 8, hd), k_cache.reshape(n_seq, n_pos, hd), v_cache.reshape(n_seq, n_pos, hd))
    return o, k_out.reshape(k_cache.shape), v_out.reshape(v_cache.shape)


N_CB = 5
N_SUB = 2
N_WB = 4
N_DB = 3
HB = 128
DB = 512


def tail_kernel(axis, o_hbm, x_hbm, wo_hbm, w1_hbm, w3_hbm, w2_hbm, ga_hbm, gm_hbm, y_ref,
                on, ob, xp, hb, src, recv0, recv1, recv2, act, wob, wb, w2b, ga_ref, gm_ref,
                o_sem, x_sem, wo_sem, wb_sem, w2_sem, gain_sem, s_sem, r_sem, g_ssem, g_rsem):
    n_steps, n_seq, d_model = x_hbm.shape
    piece = n_seq // 8
    sub_rows = piece // N_SUB
    cw = d_model // N_CB
    n_hid = w1_hbm.shape[1]
    n_j = n_hid // HB
    n_d = d_model // DB
    per_cb = n_d // N_CB
    hd = o_hbm.shape[1]
    n_heads = wo_hbm.shape[0] // hd

    me = lax.axis_index(axis)
    core = lax.rem(me, 2)
    xb = lax.rem(me // 2, 2)
    yb = me // 4
    first_bit = core * yb + (1 - core) * xb
    second_bit = core * xb + (1 - core) * yb
    fw = 1 + core
    sw = 2 - core
    partner = me + 1 - 2 * core
    fpeer = me + (1 - 2 * first_bit) * 2 * fw
    speer = me + (1 - 2 * second_bit) * 2 * sw
    fspeer = fpeer + speer - me

    def remote(src_ref, dst_ref, send, recv, dev):
        return pltpu.make_async_remote_copy(src_ref=src_ref, dst_ref=dst_ref, send_sem=send, recv_sem=recv, device_id={axis: dev}, device_id_type=MESH_ID)

    o_copy = pltpu.make_async_copy(o_hbm, on, o_sem)
    o_copy.start()

    def wo_copy(cb):
        cols = pl.ds(pl.multiple_of(cb * cw, cw), cw)
        return pltpu.make_async_copy(wo_hbm.at[:, cols], wob.at[:, cols], wo_sem.at[cb])

    for cb in range(N_CB):
        wo_copy(cb).start()
    gain_copies = (pltpu.make_async_copy(ga_hbm, ga_ref, gain_sem.at[0]), pltpu.make_async_copy(gm_hbm, gm_ref, gain_sem.at[1]))
    for cp in gain_copies:
        cp.start()
    x_copy = pltpu.make_async_copy(x_hbm.at[:, pl.ds(pl.multiple_of(piece * me, piece), piece), :], xp, x_sem)
    x_copy.start()

    def wb_copies(j, s):
        col = pl.ds(pl.multiple_of(j * HB, HB), HB)
        return (pltpu.make_async_copy(w1_hbm.at[:, col], wb.at[s, :, 0:HB], wb_sem.at[s, 0]),
                pltpu.make_async_copy(w3_hbm.at[:, col], wb.at[s, :, HB:2 * HB], wb_sem.at[s, 1]))

    def w2_copy(j, s):
        return pltpu.make_async_copy(w2_hbm.at[:, pl.ds(pl.multiple_of(j * DB, DB), DB)], w2b.at[s], w2_sem.at[s])

    def start_wb():
        for s in range(N_WB - 1):
            for cp in wb_copies(s, s):
                cp.start()

    bar = pltpu.get_barrier_semaphore()
    for dev in (partner, fpeer, speer):
        pl.semaphore_signal(bar, inc=1, device_id={axis: dev}, device_id_type=MESH_ID)
    pl.semaphore_wait(bar, 3)

    def cols_of(cb):
        return pl.ds(pl.multiple_of(cb * cw, cw), cw)

    def copy0(inst, cb):
        c = inst % n_steps
        return remote(src.at[c, :, 1 - core, :, cols_of(cb)], recv0.at[c, :, :, cols_of(cb)], s_sem.at[inst, 0, cb], r_sem.at[inst, 0, cb], partner)

    def copy1(inst, cb, k):
        c = inst % n_steps
        sb = (1 - second_bit) if k == 0 else second_bit
        idx = (1 - first_bit) * fw + sb * sw
        return remote(recv0.at[c, idx, :, cols_of(cb)], recv1.at[c, k, :, cols_of(cb)], s_sem.at[inst, 1 + k, cb], r_sem.at[inst, 1 + k, cb], fpeer)

    def copy2(inst, cb):
        c = inst % n_steps
        return remote(recv1.at[c, 0, :, cols_of(cb)], recv2.at[c, :, cols_of(cb)], s_sem.at[inst, 3, cb], r_sem.at[inst, 3, cb], speer)

    def f32(v):
        return v.astype(jnp.float32)

    def event1(inst, cb):
        c = inst % n_steps
        copy0(inst, cb).wait_recv()
        cols = cols_of(cb)

        def add(i, _):
            recv0[c, i, :, cols] = src[c, i, core, :, cols] + recv0[c, i, :, cols]
            return 0

        lax.fori_loop(0, 4, add, 0)
        copy1(inst, cb, 0).start()
        copy1(inst, cb, 1).start()

    def event2(inst, cb):
        c = inst % n_steps
        copy1(inst, cb, 0).wait_recv()
        cols = cols_of(cb)
        idx = first_bit * fw + (1 - second_bit) * sw
        recv1[c, 0, :, cols] = recv0[c, idx, :, cols] + recv1[c, 0, :, cols]
        copy2(inst, cb).start()

    def event3(inst, cb):
        c = inst % n_steps
        copy1(inst, cb, 1).wait_recv()
        copy2(inst, cb).wait_recv()
        cols = cols_of(cb)
        idx = first_bit * fw + second_bit * sw
        recv2[c, :, cols] = (f32(recv0[c, idx, :, cols]) + f32(recv1[c, 1, :, cols]) + f32(recv2[c, :, cols])).astype(jnp.bfloat16)

    def gcopy(inst, k, sub):
        c = inst % n_steps
        who, dev = ((me, speer), (me, fpeer), (me, partner), (speer, fpeer), (speer, partner), (fpeer, partner), (fspeer, partner))[k]
        part = hb.at[c, pl.ds(pl.multiple_of(who * piece + sub * sub_rows, sub_rows), sub_rows), :]
        return remote(part, part, g_ssem.at[inst, k, sub], g_rsem.at[inst, k, sub], dev)

    def event4(inst, sub):
        c = inst % n_steps
        attn = inst < n_steps

        @pl.when(sub == 0)
        def _():
            def drain(cb, _):
                copy0(inst, cb).wait_send()
                copy1(inst, cb, 0).wait_send()
                copy1(inst, cb, 1).wait_send()
                copy2(inst, cb).wait_send()
                return 0

            lax.fori_loop(0, N_CB, drain, 0)

        r = pl.ds(pl.multiple_of(sub * sub_rows, sub_rows), sub_rows)
        hr = pl.ds(pl.multiple_of(me * piece + sub * sub_rows, sub_rows), sub_rows)
        a = f32(recv2[c, r, :])
        factor = rms_factor(jnp.sum(a * a, axis=-1, keepdims=True), d_model)
        base = f32(xp[c, r, :]) if attn else f32(hb[c, hr, :])
        gain = f32((ga_ref if attn else gm_ref)[...]).reshape(1, d_model)
        hb[c, hr, :] = (base + a * factor * gain).astype(jnp.bfloat16)
        for k in (1, 0, 2):
            gcopy(inst, k, sub).start()

    def event5(inst, sub):
        gcopy(inst, 0, sub).wait_recv()
        gcopy(inst, 3, sub).start()
        gcopy(inst, 4, sub).start()
        gcopy(inst, 1, sub).wait_recv()
        gcopy(inst, 5, sub).start()

    def event7(inst, sub):
        gcopy(inst, 3, sub).wait_recv()
        gcopy(inst, 6, sub).start()

    def event8(inst, sub):
        for k in (2, 4, 5, 6):
            gcopy(inst, k, sub).wait_recv()
        for k in range(7):
            gcopy(inst, k, sub).wait_send()

    def run(j, table):
        for event, inst, start, every, count in table:
            k = j - start
            cond = (k >= 0) & (k < every * count)
            if every > 1:
                cond = cond & (lax.rem(k, every) == 0)

            @pl.when(cond)
            def _():
                event(inst, k // every)

    def loop(n, fn):
        lax.fori_loop(0, n, lambda i, _: (fn(i), 0)[1], 0)

    def out_proj(c):
        for g in range(n_heads):
            ob[:, g * hd:(g + 1) * hd] = on[pl.ds(c * n_heads + g, n_seq, stride=16), :].astype(jnp.bfloat16)

        def step(cb):
            if c == 0:
                wo_copy(cb).wait()
            part = jnp.dot(ob[...], wob[:, cols_of(cb)], preferred_element_type=jnp.float32).astype(jnp.bfloat16)
            src[c, :, :, :, cols_of(cb)] = part.reshape(4, 2, piece, cw)
            copy0(c, cb).start()

        loop(N_CB, step)

    def y_store(c):
        def step(i):
            r = pl.ds(pl.multiple_of(i * piece, piece), piece)
            y_ref[c, r, :] = hb[c, r, :]

        loop(8, step)

    o_copy.wait()
    out_proj(0)
    start_wb()
    loop(N_CB, functools.partial(event1, 0))
    out_proj(1)
    out_proj(2)
    x_copy.wait()
    for cp in gain_copies:
        cp.wait()

    def finish_reduce(inst):
        def step(k):
            @pl.when(k < N_CB)
            def _():
                event2(inst, k)

            @pl.when(k > 0)
            def _():
                event3(inst, k - 1)

        loop(N_CB + 1, step)

    def finish_gather(inst):
        loop(N_SUB, functools.partial(event4, inst))
        loop(N_SUB, functools.partial(event5, inst))
        loop(N_SUB, functools.partial(event7, inst))
        loop(N_SUB, functools.partial(event8, inst))

    finish_reduce(0)
    finish_gather(0)

    gate_tables = (
        ((event1, 1, 0, 1, N_CB), (event2, 1, 4, 2, N_CB), (event3, 1, 9, 2, N_CB), (event4, 1, 18, 1, N_SUB), (event1, 2, 20, 1, N_CB)),
        ((event1, 3, 0, 1, N_CB), (event2, 3, 6, 3, N_CB), (event5, 2, 10, 1, N_SUB), (event3, 3, 10, 3, N_CB), (event7, 2, 17, 1, N_SUB), (event8, 2, 20, 1, N_SUB), (event4, 3, 24, 1, N_SUB)),
        ((event1, 4, 0, 1, N_CB), (event7, 3, 2, 1, N_SUB), (event2, 4, 6, 2, N_CB), (event8, 3, 7, 1, N_SUB), (event3, 4, 10, 2, N_CB), (event4, 4, 19, 1, N_SUB)),
    )
    down_tables = (
        ((event2, 2, 0, 1, N_CB), (event3, 2, 4, 1, N_CB), (event5, 1, 3, 1, N_SUB), (event7, 1, 7, 1, N_SUB), (event8, 1, 9, 1, 1)),
        ((event5, 3, 6, 1, N_SUB),),
        ((event5, 4, 3, 1, N_SUB), (event7, 4, 6, 1, N_SUB), (event8, 4, 8, 1, N_SUB)),
    )
    for c in range(n_steps):
        def gate_up(j):
            s = lax.rem(j, N_WB)

            @pl.when(j + N_WB - 1 < n_j)
            def _():
                for cp in wb_copies(j + N_WB - 1, lax.rem(j + N_WB - 1, N_WB)):
                    cp.start()

            for cp in wb_copies(j, s):
                cp.wait()
            both = jnp.dot(hb[c], wb[s], preferred_element_type=jnp.float32)
            gate = both[:, :HB]
            act[:, pl.ds(pl.multiple_of(j * HB, HB), HB)] = (jax.nn.silu(gate) * both[:, HB:]).astype(jnp.bfloat16)
            run(j, gate_tables[c])

        def down(j):
            s = lax.rem(j, N_DB)

            @pl.when(j + N_DB - 1 < n_d)
            def _():
                w2_copy(j + N_DB - 1, lax.rem(j + N_DB - 1, N_DB)).start()

            w2_copy(j, s).wait()
            part = jnp.dot(act[...], w2b[s], preferred_element_type=jnp.float32).astype(jnp.bfloat16)
            src[c, :, :, :, pl.ds(pl.multiple_of(j * DB, DB), DB)] = part.reshape(4, 2, piece, DB)

            @pl.when(lax.rem(j, per_cb) == per_cb - 1)
            def _():
                copy0(n_steps + c, j // per_cb).start()

            run(j, down_tables[c])
            if c == n_steps - 1:
                run(j, ((event1, n_steps + c, 2, 2, 4), (event2, n_steps + c, 5, 2, 3), (event3, n_steps + c, 8, 2, 1)))

        for s in range(N_DB - 1):
            w2_copy(s, s).start()
        loop(n_j, gate_up)
        if c < n_steps - 1:
            start_wb()
        loop(n_d, down)
        if c == 0:
            event8(1, 1)
            event4(2, 0)
            event4(2, 1)

    last = 2 * n_steps - 1
    event1(last, 4)
    event2(last, 3)
    event3(last, 1)
    event3(last, 2)
    event2(last, 4)
    event3(last, 3)
    event3(last, 4)
    loop(N_SUB, functools.partial(event4, last))
    for c in range(n_steps - 1):
        y_store(c)
    loop(N_SUB, functools.partial(event5, last))
    loop(N_SUB, functools.partial(event7, last))
    loop(N_SUB, functools.partial(event8, last))
    y_store(n_steps - 1)


def tail_layer(o, x_seq, w_o, w_gate, w_up, w_down, g_attn, g_mlp, axis):
    n_steps, n_seq, d_model = x_seq.shape
    piece = n_seq // 8
    n_hid = w_gate.shape[1]
    bf16 = jnp.bfloat16
    anym = pl.BlockSpec(memory_space=pl.ANY)
    dma = pltpu.SemaphoreType.DMA
    return pl.pallas_call(
        functools.partial(tail_kernel, axis),
        out_shape=pltpu.VMEM((n_steps, n_seq, d_model), bf16),
        in_specs=[anym] * 8,
        out_specs=pl.BlockSpec(memory_space=pltpu.VMEM),
        scratch_shapes=[
            pltpu.VMEM(o.shape, jnp.float32),
            pltpu.VMEM((n_seq, w_o.shape[0]), bf16),
            pltpu.VMEM((n_steps, piece, d_model), bf16),
            pltpu.VMEM((n_steps, n_seq, d_model), bf16),
            pltpu.VMEM((n_steps, 4, 2, piece, d_model), bf16),
            pltpu.VMEM((n_steps, 4, piece, d_model), bf16),
            pltpu.VMEM((n_steps, 2, piece, d_model), bf16),
            pltpu.VMEM((n_steps, piece, d_model), bf16),
            pltpu.VMEM((n_seq, n_hid), bf16),
            pltpu.VMEM(w_o.shape, bf16),
            pltpu.VMEM((N_WB, d_model, 2 * HB), bf16),
            pltpu.VMEM((N_DB, n_hid, DB), bf16),
            pltpu.VMEM((d_model,), bf16),
            pltpu.VMEM((d_model,), bf16),
            dma, dma, dma((N_CB,)), dma((N_WB, 2)), dma((N_DB,)), dma((2,)),
            dma((2 * n_steps, 4, N_CB)), dma((2 * n_steps, 4, N_CB)), dma((2 * n_steps, 7, N_SUB)), dma((2 * n_steps, 7, N_SUB)),
        ],
        compiler_params=pltpu.CompilerParams(collective_id=1, has_side_effects=True, vmem_limit_bytes=55 * MIB),
    )(o, x_seq, w_o, w_gate, w_up, w_down, g_attn, g_mlp)


def layer_steps(x_seq, cache_len, k_cache, v_cache, w_q, w_k, w_v, w_o, w_gate, w_up, w_down, g_q, g_k, g_attn, g_mlp, q_width, kv_width):
    n_steps, n_seq, _ = x_seq.shape
    hd = k_cache.shape[-1]
    q, kv = head_layer(x_seq, cache_len, w_q, w_k, w_v, g_q, g_k, q_width, kv_width, 'tp')
    o, k_out, v_out = attn_layer(cache_len, q, kv, k_cache, v_cache, w_q.shape[1] // hd, n_steps)
    y = tail_layer(o.reshape(n_seq * 16, hd), x_seq, w_o, w_gate, w_up, w_down, g_attn, g_mlp, 'tp')
    return y, k_out, v_out


def solution(mesh):
    tp_size = mesh.shape['tp']

    def local_run(x_seq, cache_len, k_cache, v_cache, w_q, w_k, w_v, w_o, w_gate, w_up, w_down, g_q, g_k, g_attn, g_mlp):
        return layer_steps(x_seq, cache_len, k_cache, v_cache, w_q, w_k, w_v, w_o, w_gate, w_up, w_down, g_q, g_k, g_attn, g_mlp, w_q.shape[1] * tp_size, w_k.shape[1] * tp_size)

    data_spec = P(None, 'dp', None)
    cache_spec = P('dp', 'tp', None, None)
    col_spec = P(None, 'tp')
    row_spec = P('tp', None)
    arg_specs = (data_spec, P('dp'), cache_spec, cache_spec, col_spec, col_spec, col_spec, row_spec, col_spec, col_spec, row_spec, P('tp'), P('tp'), P(None), P(None))
    out_specs = (data_spec, cache_spec, cache_spec)
    return jax.shard_map(local_run, mesh=mesh, in_specs=arg_specs, out_specs=out_specs, check_vma=False)
```

```python
import functools

import jax
import jax.numpy as jnp
import numpy as np
from jax import lax
from jax.experimental import pallas as pl
from jax.experimental.pallas import tpu as pltpu
from jax.sharding import PartitionSpec as P

ROPE_THETA = 500000.0
NORM_EPS = 1e-6
MESH_ID = pl.DeviceIdType.MESH
MIB = 2**20


def rms_factor(sq_sum, full_width):
    return lax.rsqrt(sq_sum / full_width + NORM_EPS)


N_KB = 5


def head_kernel(axis, q_width, kv_width, x_hbm, wq_hbm, wk_hbm, wv_hbm, gq_hbm, gk_hbm, len_hbm, freq_hbm, q_ref, kv_ref,
                xv, wv, acc, raw, sums, parts, gq_ref, gk_ref, len_ref, freq_ref, in_sem, small_sem, s_sem, r_sem):
    n_steps, n_seq, d_model = x_hbm.shape
    wq_cols = wq_hbm.shape[1]
    hd = wk_hbm.shape[1]
    n_heads = wq_cols // hd
    kw = d_model // N_KB
    n_blk = n_steps * 2
    me = lax.axis_index(axis)

    def in_copies(kb):
        ks = pl.ds(pl.multiple_of(kb * kw, kw), kw)
        return (pltpu.make_async_copy(x_hbm.at[:, :, ks], xv.at[:, :, ks], in_sem.at[kb, 0]),
                pltpu.make_async_copy(wq_hbm.at[ks, :], wv.at[ks, 0:wq_cols], in_sem.at[kb, 1]),
                pltpu.make_async_copy(wk_hbm.at[ks, :], wv.at[ks, wq_cols:wq_cols + hd], in_sem.at[kb, 2]),
                pltpu.make_async_copy(wv_hbm.at[ks, :], wv.at[ks, wq_cols + hd:wq_cols + 2 * hd], in_sem.at[kb, 3]))

    for kb in range(N_KB):
        for cp in in_copies(kb):
            cp.start()

    small = [pltpu.make_async_copy(hbm, vmem, small_sem.at[n]) for n, (hbm, vmem) in enumerate(((gq_hbm, gq_ref), (gk_hbm, gk_ref), (len_hbm, len_ref), (freq_hbm, freq_ref)))]
    for cp in small:
        cp.start()

    bar = pltpu.get_barrier_semaphore()
    for i in range(1, 8):
        pl.semaphore_signal(bar, inc=1, device_id={axis: lax.rem(me + i, 8)}, device_id_type=MESH_ID)

    def project(kb, _):
        for cp in in_copies(kb):
            cp.wait()
        ks = pl.ds(pl.multiple_of(kb * kw, kw), kw)
        for t in range(n_steps):
            acc[t] += jnp.dot(xv[t, :, ks], wv[ks, :], preferred_element_type=jnp.float32)
        return 0

    acc[...] = jnp.zeros_like(acc)
    lax.fori_loop(0, N_KB, project, 0)

    lane = lax.broadcasted_iota(jnp.int32, (128, 128), 1)
    diag = lane == lax.broadcasted_iota(jnp.int32, (128, 128), 0)

    def to_row(col):
        return jnp.sum(jnp.where(diag, jnp.broadcast_to(col, (128, 128)), 0.0), axis=0, keepdims=True)

    def to_col(row):
        return jnp.sum(jnp.where(diag, jnp.broadcast_to(row, (128, 128)), 0.0), axis=1, keepdims=True)

    def rounded(v):
        return v.astype(jnp.bfloat16).astype(jnp.float32)

    sums[...] = jnp.zeros_like(sums)
    for blk in range(n_blk):
        t, half = blk // 2, blk % 2
        rows = slice(half * 128, half * 128 + 128)
        sq = None
        for g in range(n_heads):
            val = rounded(acc[t, rows, g * hd:(g + 1) * hd])
            raw[blk, g] = val
            sq = val * val if sq is None else sq + val * val
        sums[blk:blk + 1, :] = to_row(jnp.sum(sq, axis=-1, keepdims=True))
        val = rounded(acc[t, rows, wq_cols:wq_cols + hd])
        raw[blk, n_heads] = val
        sums[n_blk + blk:n_blk + blk + 1, :] = to_row(jnp.sum(val * val, axis=-1, keepdims=True))

    def exchange(i):
        return pltpu.make_async_remote_copy(src_ref=sums, dst_ref=parts.at[me], send_sem=s_sem.at[i - 1], recv_sem=r_sem.at[i - 1], device_id={axis: lax.rem(me + i, 8)}, device_id_type=MESH_ID)

    pl.semaphore_wait(bar, 7)
    for i in range(1, 8):
        exchange(i).start()
    parts[me] = sums[...]

    for blk in range(n_blk):
        t, half = blk // 2, blk % 2
        rows = slice(half * 128, half * 128 + 128)
        kv_ref[pl.ds(half * 1024 + 3 + t, 128, stride=8), :] = rounded(acc[t, rows, wq_cols + hd:wq_cols + 2 * hd])
    for half in range(2):
        zero = jnp.zeros((128, hd), jnp.float32)
        for slot in range(n_steps * n_heads, 16):
            q_ref[pl.ds(half * 2048 + slot, 128, stride=16), :] = zero
        for slot in range(2 * n_steps, 8):
            kv_ref[pl.ds(half * 1024 + slot, 128, stride=8), :] = zero
    for cp in small:
        cp.wait()
    low = lane < 64
    freq = freq_ref[...]
    lens = len_ref[...].astype(jnp.float32)
    angle = jnp.where(low, to_col(lens[0:1, :]), to_col(lens[1:2, :])) * freq
    cos_p = jnp.cos(angle)
    sin_p = jnp.sin(angle)
    cos_r = pltpu.roll(cos_p, 64, 1)
    sin_r = pltpu.roll(sin_p, 64, 1)
    cos_0 = (jnp.where(low, cos_p, cos_r), jnp.where(low, cos_r, cos_p))
    sin_0 = (jnp.where(low, sin_p, sin_r), jnp.where(low, sin_r, sin_p))

    for i in range(1, 8):
        exchange(i).wait()
    total = parts[0]
    for i in range(1, 8):
        total = total + parts[i]
    q_fac = rms_factor(total[0:n_blk], q_width)
    k_fac = rms_factor(total[n_blk:2 * n_blk], kv_width)
    gain_q = gq_ref[...].astype(jnp.float32).reshape(1, wq_cols)
    gain_k = gk_ref[...].astype(jnp.float32).reshape(1, hd)

    for blk in range(n_blk):
        t, half = blk // 2, blk % 2
        if t == 0:
            cos_t, sin_t = cos_0[half], sin_0[half]
        else:
            cos_s, sin_s = jnp.cos(freq * float(t)), jnp.sin(freq * float(t))
            cos_t = cos_0[half] * cos_s - sin_0[half] * sin_s
            sin_t = sin_0[half] * cos_s + cos_0[half] * sin_s
        sin_t = jnp.where(low, -sin_t, sin_t)

        def rope(val):
            return rounded(val * cos_t + pltpu.roll(val, 64, 1) * sin_t)

        fac = to_col(q_fac[blk:blk + 1, :])
        for g in range(n_heads):
            q_ref[pl.ds(half * 2048 + t * n_heads + g, 128, stride=16), :] = rope(raw[blk, g] * fac * gain_q[:, g * hd:(g + 1) * hd])
        fac = to_col(k_fac[blk:blk + 1, :])
        kv_ref[pl.ds(half * 1024 + t, 128, stride=8), :] = rope(raw[blk, n_heads] * fac * gain_k)


def head_layer(x_seq, cache_len, w_q, w_k, w_v, g_q, g_k, q_width, kv_width, axis):
    n_steps, n_seq, d_model = x_seq.shape
    hd = w_k.shape[1]
    cols = w_q.shape[1] + 2 * hd
    half_dim = hd // 2
    bf16, f32 = jnp.bfloat16, jnp.float32
    inv_freq = ROPE_THETA ** (-(np.arange(half_dim) * (2.0 / hd)))
    freq = jnp.asarray(np.concatenate([inv_freq, inv_freq]).reshape(1, hd), dtype=f32)
    anym = pl.BlockSpec(memory_space=pl.ANY)
    vmem = pl.BlockSpec(memory_space=pltpu.VMEM)
    dma = pltpu.SemaphoreType.DMA
    return pl.pallas_call(
        functools.partial(head_kernel, axis, q_width, kv_width),
        out_shape=(jax.ShapeDtypeStruct((n_seq * 16, hd), f32), jax.ShapeDtypeStruct((n_seq * 8, hd), f32)),
        in_specs=[anym] * 8,
        out_specs=(vmem, vmem),
        scratch_shapes=[
            pltpu.VMEM((n_steps, n_seq, d_model), bf16),
            pltpu.VMEM((d_model, cols), bf16),
            pltpu.VMEM((n_steps, n_seq, cols), f32),
            pltpu.VMEM((2 * n_steps, w_q.shape[1] // hd + 1, 128, hd), f32),
            pltpu.VMEM((16, 128), f32),
            pltpu.VMEM((8, 16, 128), f32),
            pltpu.VMEM(g_q.shape, bf16),
            pltpu.VMEM(g_k.shape, bf16),
            pltpu.VMEM((2, n_seq // 2), jnp.int32),
            pltpu.VMEM((1, hd), f32),
            dma((N_KB, 4)), dma((4,)), dma((7,)), dma((7,)),
        ],
        compiler_params=pltpu.CompilerParams(collective_id=0, has_side_effects=True, vmem_limit_bytes=63 * MIB),
    )(x_seq, w_q, w_k, w_v, g_q, g_k, cache_len.reshape(2, n_seq // 2), freq)


SEQ_GRP = 16
N_RING = 8
AHEAD = 4


def attn_kernel(n_heads, n_steps, len_ref, q_hbm, kv_hbm, k_hbm, v_hbm, o_hbm, ko_hbm, vo_hbm, qb, kvb, kb, vb, ob, in_sem, out_sem):
    n_seq, n_pos, hd = k_hbm.shape
    n_grp = n_seq // SEQ_GRP
    fixed = n_pos // 2
    scale = hd ** -0.5
    row = lax.broadcasted_iota(jnp.int32, (n_pos - fixed, hd), 0)
    s_step = lax.broadcasted_iota(jnp.int32, (16, n_pos - fixed), 0) // n_heads
    s_last = lax.broadcasted_iota(jnp.int32, (16, n_pos - fixed), 1) + fixed - s_step

    def copies(grp, pairs, sem):
        seqs = pl.ds(grp * SEQ_GRP, SEQ_GRP)
        s = lax.rem(grp, N_RING)
        return [pltpu.make_async_copy(hbm.at[seqs], vmem.at[s], sem.at[s, n]) if sem is in_sem else pltpu.make_async_copy(vmem.at[s], hbm.at[seqs], sem.at[s, n]) for n, (hbm, vmem) in enumerate(pairs)]

    def loads(grp):
        return copies(grp, ((k_hbm, kb), (v_hbm, vb), (q_hbm, qb), (kv_hbm, kvb)), in_sem)

    def stores(grp):
        return copies(grp, ((ko_hbm, kb), (vo_hbm, vb), (o_hbm, ob)), out_sem)

    for grp in range(AHEAD):
        for cp in loads(grp):
            cp.start()

    def group(grp, _):
        slot = lax.rem(grp, N_RING)

        @pl.when(grp + AHEAD < n_grp)
        def _():
            @pl.when(grp + AHEAD >= N_RING)
            def _():
                for cp in stores(grp + AHEAD - N_RING):
                    cp.wait()

            for cp in loads(grp + AHEAD):
                cp.start()

        for cp in loads(grp):
            cp.wait()
        idx = range(SEQ_GRP)
        lens = [len_ref[grp * SEQ_GRP + i] for i in idx]
        for i, length in zip(idx, lens):
            rel = row - (length - fixed)
            for buf, first in ((kb, 0), (vb, n_steps)):
                vals = buf[slot, i, fixed:n_pos, :].astype(jnp.float32)
                for t in range(n_steps):
                    vals = jnp.where(rel == t, kvb[slot, i, first + t:first + t + 1, :], vals)
                buf[slot, i, fixed:n_pos, :] = vals.astype(jnp.bfloat16)
        scores = [lax.dot_general(qb[slot, i].astype(jnp.bfloat16), kb[slot, i], (((1,), (1,)), ((), ())), preferred_element_type=jnp.float32) for i in idx]
        probs = []
        sums = []
        for s, length in zip(scores, lens):
            lo = s[:, 0:fixed] * scale
            hi = jnp.where(s_last <= length, s[:, fixed:n_pos] * scale, -jnp.inf)
            top = jnp.max(jnp.maximum(lo, hi), axis=-1, keepdims=True)
            lo = jnp.exp(lo - top)
            hi = jnp.exp(hi - top)
            sums.append(jnp.sum(lo + hi, axis=-1, keepdims=True))
            probs.append(jnp.concatenate([lo.astype(jnp.bfloat16), hi.astype(jnp.bfloat16)], axis=-1))
        for i, p, total in zip(idx, probs, sums):
            ob[slot, i] = jnp.dot(p, vb[slot, i], preferred_element_type=jnp.float32) / total
        for cp in stores(grp):
            cp.start()
        return 0

    lax.fori_loop(0, n_grp, group, 0)

    def drain(grp, _):
        for cp in stores(grp):
            cp.wait()
        return 0

    lax.fori_loop(n_grp - N_RING, n_grp, drain, 0)


def attn_layer(cache_len, q, kv, k_cache, v_cache, n_heads, n_steps):
    n_seq, _, n_pos, hd = k_cache.shape
    bf16, f32 = jnp.bfloat16, jnp.float32
    anym = pl.BlockSpec(memory_space=pl.ANY)
    dma = pltpu.SemaphoreType.DMA
    ring = (N_RING, SEQ_GRP)
    o, k_out, v_out = pl.pallas_call(
        functools.partial(attn_kernel, n_heads, n_steps),
        out_shape=(jax.ShapeDtypeStruct((n_seq, 16, hd), f32), jax.ShapeDtypeStruct((n_seq, n_pos, hd), bf16), jax.ShapeDtypeStruct((n_seq, n_pos, hd), bf16)),
        in_specs=[pl.BlockSpec(memory_space=pltpu.SMEM)] + [anym] * 4,
        out_specs=(anym, anym, anym),
        scratch_shapes=[
            pltpu.VMEM(ring + (16, hd), f32),
            pltpu.VMEM(ring + (8, hd), f32),
            pltpu.VMEM(ring + (n_pos, hd), bf16),
            pltpu.VMEM(ring + (n_pos, hd), bf16),
            pltpu.VMEM(ring + (16, hd), f32),
            dma((N_RING, 4)), dma((N_RING, 3)),
        ],
        compiler_params=pltpu.CompilerParams(vmem_limit_bytes=63 * MIB),
    )(cache_len, q.reshape(n_seq, 16, hd), kv.reshape(n_seq, 8, hd), k_cache.reshape(n_seq, n_pos, hd), v_cache.reshape(n_seq, n_pos, hd))
    return o, k_out.reshape(k_cache.shape), v_out.reshape(v_cache.shape)


N_CB = 5
N_SUB = 2
N_WB = 4
N_DB = 3
HB = 128
DB = 512


def tail_kernel(axis, o_hbm, x_hbm, wo_hbm, w1_hbm, w3_hbm, w2_hbm, ga_hbm, gm_hbm, y_ref,
                on, ob, xp, hb, src, recv0, recv1, recv2, act, wob, wb, w2b, ga_ref, gm_ref,
                o_sem, x_sem, wo_sem, wb_sem, w2_sem, gain_sem, s_sem, r_sem, g_ssem, g_rsem):
    n_steps, n_seq, d_model = x_hbm.shape
    piece = n_seq // 8
    sub_rows = piece // N_SUB
    cw = d_model // N_CB
    n_hid = w1_hbm.shape[1]
    n_j = n_hid // HB
    n_d = d_model // DB
    per_cb = n_d // N_CB
    hd = o_hbm.shape[1]
    n_heads = wo_hbm.shape[0] // hd

    me = lax.axis_index(axis)
    core = lax.rem(me, 2)
    xb = lax.rem(me // 2, 2)
    yb = me // 4
    first_bit = core * yb + (1 - core) * xb
    second_bit = core * xb + (1 - core) * yb
    fw = 1 + core
    sw = 2 - core
    partner = me + 1 - 2 * core
    fpeer = me + (1 - 2 * first_bit) * 2 * fw
    speer = me + (1 - 2 * second_bit) * 2 * sw
    fspeer = fpeer + speer - me

    def remote(src_ref, dst_ref, send, recv, dev):
        return pltpu.make_async_remote_copy(src_ref=src_ref, dst_ref=dst_ref, send_sem=send, recv_sem=recv, device_id={axis: dev}, device_id_type=MESH_ID)

    o_copy = pltpu.make_async_copy(o_hbm, on, o_sem)
    o_copy.start()

    def wo_copy(cb):
        cols = pl.ds(pl.multiple_of(cb * cw, cw), cw)
        return pltpu.make_async_copy(wo_hbm.at[:, cols], wob.at[:, cols], wo_sem.at[cb])

    for cb in range(N_CB):
        wo_copy(cb).start()
    gain_copies = (pltpu.make_async_copy(ga_hbm, ga_ref, gain_sem.at[0]), pltpu.make_async_copy(gm_hbm, gm_ref, gain_sem.at[1]))
    for cp in gain_copies:
        cp.start()
    x_copy = pltpu.make_async_copy(x_hbm.at[:, pl.ds(pl.multiple_of(piece * me, piece), piece), :], xp, x_sem)
    x_copy.start()

    def wb_copies(j, s):
        col = pl.ds(pl.multiple_of(j * HB, HB), HB)
        return (pltpu.make_async_copy(w1_hbm.at[:, col], wb.at[s, :, 0:HB], wb_sem.at[s, 0]),
                pltpu.make_async_copy(w3_hbm.at[:, col], wb.at[s, :, HB:2 * HB], wb_sem.at[s, 1]))

    def w2_copy(j, s):
        return pltpu.make_async_copy(w2_hbm.at[:, pl.ds(pl.multiple_of(j * DB, DB), DB)], w2b.at[s], w2_sem.at[s])

    def start_wb():
        for s in range(N_WB - 1):
            for cp in wb_copies(s, s):
                cp.start()

    bar = pltpu.get_barrier_semaphore()
    for dev in (partner, fpeer, speer):
        pl.semaphore_signal(bar, inc=1, device_id={axis: dev}, device_id_type=MESH_ID)
    pl.semaphore_wait(bar, 3)

    def cols_of(cb):
        return pl.ds(pl.multiple_of(cb * cw, cw), cw)

    def copy0(inst, cb):
        c = inst % n_steps
        return remote(src.at[c, :, 1 - core, :, cols_of(cb)], recv0.at[c, :, :, cols_of(cb)], s_sem.at[inst, 0, cb], r_sem.at[inst, 0, cb], partner)

    def copy1(inst, cb, k):
        c = inst % n_steps
        sb = (1 - second_bit) if k == 0 else second_bit
        idx = (1 - first_bit) * fw + sb * sw
        return remote(recv0.at[c, idx, :, cols_of(cb)], recv1.at[c, k, :, cols_of(cb)], s_sem.at[inst, 1 + k, cb], r_sem.at[inst, 1 + k, cb], fpeer)

    def copy2(inst, cb):
        c = inst % n_steps
        return remote(recv1.at[c, 0, :, cols_of(cb)], recv2.at[c, :, cols_of(cb)], s_sem.at[inst, 3, cb], r_sem.at[inst, 3, cb], speer)

    def f32(v):
        return v.astype(jnp.float32)

    def event1(inst, cb):
        c = inst % n_steps
        copy0(inst, cb).wait_recv()
        cols = cols_of(cb)

        def add(i, _):
            recv0[c, i, :, cols] = src[c, i, core, :, cols] + recv0[c, i, :, cols]
            return 0

        lax.fori_loop(0, 4, add, 0)
        copy1(inst, cb, 0).start()
        copy1(inst, cb, 1).start()

    def event2(inst, cb):
        c = inst % n_steps
        copy1(inst, cb, 0).wait_recv()
        cols = cols_of(cb)
        idx = first_bit * fw + (1 - second_bit) * sw
        recv1[c, 0, :, cols] = recv0[c, idx, :, cols] + recv1[c, 0, :, cols]
        copy2(inst, cb).start()

    def event3(inst, cb):
        c = inst % n_steps
        copy1(inst, cb, 1).wait_recv()
        copy2(inst, cb).wait_recv()
        cols = cols_of(cb)
        idx = first_bit * fw + second_bit * sw
        recv2[c, :, cols] = (f32(recv0[c, idx, :, cols]) + f32(recv1[c, 1, :, cols]) + f32(recv2[c, :, cols])).astype(jnp.bfloat16)

    def gcopy(inst, k, sub):
        c = inst % n_steps
        who, dev = ((me, speer), (me, fpeer), (me, partner), (speer, fpeer), (speer, partner), (fpeer, partner), (fspeer, partner))[k]
        part = hb.at[c, pl.ds(pl.multiple_of(who * piece + sub * sub_rows, sub_rows), sub_rows), :]
        return remote(part, part, g_ssem.at[inst, k, sub], g_rsem.at[inst, k, sub], dev)

    def event4(inst, sub):
        c = inst % n_steps
        attn = inst < n_steps

        @pl.when(sub == 0)
        def _():
            def drain(cb, _):
                copy0(inst, cb).wait_send()
                copy1(inst, cb, 0).wait_send()
                copy1(inst, cb, 1).wait_send()
                copy2(inst, cb).wait_send()
                return 0

            lax.fori_loop(0, N_CB, drain, 0)

        r = pl.ds(pl.multiple_of(sub * sub_rows, sub_rows), sub_rows)
        hr = pl.ds(pl.multiple_of(me * piece + sub * sub_rows, sub_rows), sub_rows)
        a = f32(recv2[c, r, :])
        factor = rms_factor(jnp.sum(a * a, axis=-1, keepdims=True), d_model)
        base = f32(xp[c, r, :]) if attn else f32(hb[c, hr, :])
        gain = f32((ga_ref if attn else gm_ref)[...]).reshape(1, d_model)
        hb[c, hr, :] = (base + a * factor * gain).astype(jnp.bfloat16)
        for k in (1, 0, 2):
            gcopy(inst, k, sub).start()

    def event5(inst, sub):
        gcopy(inst, 0, sub).wait_recv()
        gcopy(inst, 3, sub).start()
        gcopy(inst, 4, sub).start()
        gcopy(inst, 1, sub).wait_recv()
        gcopy(inst, 5, sub).start()

    def event7(inst, sub):
        gcopy(inst, 3, sub).wait_recv()
        gcopy(inst, 6, sub).start()

    def event8(inst, sub):
        for k in (2, 4, 5, 6):
            gcopy(inst, k, sub).wait_recv()
        for k in range(7):
            gcopy(inst, k, sub).wait_send()

    def run(j, table):
        for event, inst, start, every, count in table:
            k = j - start
            cond = (k >= 0) & (k < every * count)
            if every > 1:
                cond = cond & (lax.rem(k, every) == 0)

            @pl.when(cond)
            def _():
                event(inst, k // every)

    def loop(n, fn):
        lax.fori_loop(0, n, lambda i, _: (fn(i), 0)[1], 0)

    def out_proj(c):
        for g in range(n_heads):
            ob[:, g * hd:(g + 1) * hd] = on[pl.ds(c * n_heads + g, n_seq, stride=16), :].astype(jnp.bfloat16)

        def step(cb):
            if c == 0:
                wo_copy(cb).wait()
            part = jnp.dot(ob[...], wob[:, cols_of(cb)], preferred_element_type=jnp.float32).astype(jnp.bfloat16)
            src[c, :, :, :, cols_of(cb)] = part.reshape(4, 2, piece, cw)
            copy0(c, cb).start()

        loop(N_CB, step)

    def y_store(c):
        def step(i):
            r = pl.ds(pl.multiple_of(i * piece, piece), piece)
            y_ref[c, r, :] = hb[c, r, :]

        loop(8, step)

    o_copy.wait()
    out_proj(0)
    start_wb()
    loop(N_CB, functools.partial(event1, 0))
    out_proj(1)
    x_copy.wait()
    for cp in gain_copies:
        cp.wait()

    def finish_reduce(inst):
        def step(k):
            @pl.when(k < N_CB)
            def _():
                event2(inst, k)

            @pl.when(k > 0)
            def _():
                event3(inst, k - 1)

        loop(N_CB + 1, step)

    finish_reduce(0)
    loop(N_SUB, functools.partial(event4, 0))
    out_proj(2)
    loop(N_SUB, functools.partial(event5, 0))
    loop(N_SUB, functools.partial(event7, 0))
    loop(N_SUB, functools.partial(event8, 0))

    gate_tables = (
        ((event1, 1, 0, 1, N_CB), (event2, 1, 4, 2, N_CB), (event3, 1, 9, 2, N_CB), (event4, 1, 18, 1, N_SUB), (event1, 2, 20, 1, N_CB)),
        ((event1, 3, 0, 1, N_CB), (event2, 3, 6, 3, N_CB), (event5, 2, 10, 1, N_SUB), (event3, 3, 10, 3, N_CB), (event7, 2, 17, 1, N_SUB), (event8, 2, 20, 1, N_SUB), (event4, 3, 24, 1, N_SUB)),
        ((event1, 4, 0, 1, N_CB), (event7, 3, 2, 1, N_SUB), (event2, 4, 6, 2, N_CB), (event8, 3, 7, 1, N_SUB), (event3, 4, 10, 2, N_CB), (event4, 4, 19, 1, N_SUB)),
    )
    down_tables = (
        ((event2, 2, 0, 1, N_CB), (event3, 2, 4, 1, N_CB), (event5, 1, 3, 1, N_SUB), (event7, 1, 7, 1, N_SUB), (event8, 1, 9, 1, 1)),
        ((event5, 3, 6, 1, N_SUB),),
        ((event5, 4, 3, 1, N_SUB), (event7, 4, 6, 1, N_SUB), (event8, 4, 8, 1, N_SUB)),
    )
    for c in range(n_steps):
        def gate_up(j):
            s = lax.rem(j, N_WB)

            @pl.when(j + N_WB - 1 < n_j)
            def _():
                for cp in wb_copies(j + N_WB - 1, lax.rem(j + N_WB - 1, N_WB)):
                    cp.start()

            for cp in wb_copies(j, s):
                cp.wait()
            both = jnp.dot(hb[c], wb[s], preferred_element_type=jnp.float32)
            gate = both[:, :HB]
            act[:, pl.ds(pl.multiple_of(j * HB, HB), HB)] = (jax.nn.silu(gate) * both[:, HB:]).astype(jnp.bfloat16)
            run(j, gate_tables[c])

        def down(j):
            s = lax.rem(j, N_DB)

            @pl.when(j + N_DB - 1 < n_d)
            def _():
                w2_copy(j + N_DB - 1, lax.rem(j + N_DB - 1, N_DB)).start()

            w2_copy(j, s).wait()
            part = jnp.dot(act[...], w2b[s], preferred_element_type=jnp.float32).astype(jnp.bfloat16)
            src[c, :, :, :, pl.ds(pl.multiple_of(j * DB, DB), DB)] = part.reshape(4, 2, piece, DB)

            @pl.when(lax.rem(j, per_cb) == per_cb - 1)
            def _():
                copy0(n_steps + c, j // per_cb).start()

            run(j, down_tables[c])
            if c == n_steps - 1:
                run(j, ((event1, n_steps + c, 2, 2, 4), (event2, n_steps + c, 5, 2, 3), (event3, n_steps + c, 8, 2, 1)))

        for s in range(N_DB - 1):
            w2_copy(s, s).start()
        loop(n_j, gate_up)
        if c < n_steps - 1:
            start_wb()
        loop(n_d, down)
        if c == 0:
            event8(1, 1)
            event4(2, 0)
            event4(2, 1)

    last = 2 * n_steps - 1
    event1(last, 4)
    event2(last, 3)
    event3(last, 1)
    event3(last, 2)
    event2(last, 4)
    event3(last, 3)
    event3(last, 4)
    loop(N_SUB, functools.partial(event4, last))
    for c in range(n_steps - 1):
        y_store(c)
    loop(N_SUB, functools.partial(event5, last))
    loop(N_SUB, functools.partial(event7, last))
    loop(N_SUB, functools.partial(event8, last))
    y_store(n_steps - 1)


def tail_layer(o, x_seq, w_o, w_gate, w_up, w_down, g_attn, g_mlp, axis):
    n_steps, n_seq, d_model = x_seq.shape
    piece = n_seq // 8
    n_hid = w_gate.shape[1]
    bf16 = jnp.bfloat16
    anym = pl.BlockSpec(memory_space=pl.ANY)
    dma = pltpu.SemaphoreType.DMA
    return pl.pallas_call(
        functools.partial(tail_kernel, axis),
        out_shape=pltpu.VMEM((n_steps, n_seq, d_model), bf16),
        in_specs=[anym] * 8,
        out_specs=pl.BlockSpec(memory_space=pltpu.VMEM),
        scratch_shapes=[
            pltpu.VMEM(o.shape, jnp.float32),
            pltpu.VMEM((n_seq, w_o.shape[0]), bf16),
            pltpu.VMEM((n_steps, piece, d_model), bf16),
            pltpu.VMEM((n_steps, n_seq, d_model), bf16),
            pltpu.VMEM((n_steps, 4, 2, piece, d_model), bf16),
            pltpu.VMEM((n_steps, 4, piece, d_model), bf16),
            pltpu.VMEM((n_steps, 2, piece, d_model), bf16),
            pltpu.VMEM((n_steps, piece, d_model), bf16),
            pltpu.VMEM((n_seq, n_hid), bf16),
            pltpu.VMEM(w_o.shape, bf16),
            pltpu.VMEM((N_WB, d_model, 2 * HB), bf16),
            pltpu.VMEM((N_DB, n_hid, DB), bf16),
            pltpu.VMEM((d_model,), bf16),
            pltpu.VMEM((d_model,), bf16),
            dma, dma, dma((N_CB,)), dma((N_WB, 2)), dma((N_DB,)), dma((2,)),
            dma((2 * n_steps, 4, N_CB)), dma((2 * n_steps, 4, N_CB)), dma((2 * n_steps, 7, N_SUB)), dma((2 * n_steps, 7, N_SUB)),
        ],
        compiler_params=pltpu.CompilerParams(collective_id=1, has_side_effects=True, vmem_limit_bytes=55 * MIB),
    )(o, x_seq, w_o, w_gate, w_up, w_down, g_attn, g_mlp)


def layer_steps(x_seq, cache_len, k_cache, v_cache, w_q, w_k, w_v, w_o, w_gate, w_up, w_down, g_q, g_k, g_attn, g_mlp, q_width, kv_width):
    n_steps, n_seq, _ = x_seq.shape
    hd = k_cache.shape[-1]
    q, kv = head_layer(x_seq, cache_len, w_q, w_k, w_v, g_q, g_k, q_width, kv_width, 'tp')
    o, k_out, v_out = attn_layer(cache_len, q, kv, k_cache, v_cache, w_q.shape[1] // hd, n_steps)
    y = tail_layer(o.reshape(n_seq * 16, hd), x_seq, w_o, w_gate, w_up, w_down, g_attn, g_mlp, 'tp')
    return y, k_out, v_out


def solution(mesh):
    tp_size = mesh.shape['tp']

    def local_run(x_seq, cache_len, k_cache, v_cache, w_q, w_k, w_v, w_o, w_gate, w_up, w_down, g_q, g_k, g_attn, g_mlp):
        return layer_steps(x_seq, cache_len, k_cache, v_cache, w_q, w_k, w_v, w_o, w_gate, w_up, w_down, g_q, g_k, g_attn, g_mlp, w_q.shape[1] * tp_size, w_k.shape[1] * tp_size)

    data_spec = P(None, 'dp', None)
    cache_spec = P('dp', 'tp', None, None)
    col_spec = P(None, 'tp')
    row_spec = P('tp', None)
    arg_specs = (data_spec, P('dp'), cache_spec, cache_spec, col_spec, col_spec, col_spec, row_spec, col_spec, col_spec, row_spec, P('tp'), P('tp'), P(None), P(None))
    out_specs = (data_spec, cache_spec, cache_spec)
    return jax.shard_map(local_run, mesh=mesh, in_specs=arg_specs, out_specs=out_specs, check_vma=False)
```
